128 devices in a mesh: gx: 8 (over y_lo, x), gy: 8 (over z, core), gz: 2 (over y_hi).
Axes of the slice: x: 4, y: 4 (y_hi: 2, y_lo: 2; y = y_hi * 2 + y_lo), z: 4, core: 2. Of those that a mesh axis runs over, the one named last changes fastest.
Arguments:
- blocks: int32 [131072, 4], P(('gx', 'gy', 'gz')), may hold values from 0 to 15, as said below
- coefficients: bfloat16 [131072, 4, 128], P(('gx', 'gy', 'gz')), may hold values from -80 to 80
- residuals: float32 [131072], P(('gx', 'gy', 'gz')), may hold values from -3000 to 3000
Outputs:
- factor: float32 [8, 2, 128, 8, 2, 128], P('gx', None, None, 'gy')
- solution: float32 [16, 128], replicated
The draws below stay inside these ranges and needn't reach their ends.
Inputs may be any that keep to these rules, and one draw needn't show every extreme that they name: Each row names 4 different blocks.
All inputs are finite; a program needn't handle non-finite values.
Results may differ from the reference program's by a relative error of at most 0.0003.
Values sent between devices are 32-bit elements; how exact they have to be, the bound alone decides.
A program may use at most 128 MiB of HBM per device.

```python
import math
import jax
import jax.numpy as jnp
from jax import lax

G = 2048
BS = 128
SLOTS = 4
OBS = 131072
N_GX = 8
N_GY = 8


def pick_blocks(key):
    nblock = G // BS
    base = jax.random.fold_in(key, 11)
    scores = jax.random.randint(base, (OBS, nblock), 0, 1 << 20) * nblock + jnp.arange(nblock, dtype=jnp.int32)[None, :]
    chosen = lax.top_k(scores, SLOTS)[1]
    return chosen.astype(jnp.int32)


def make_coefficients(key):
    base = jax.random.fold_in(key, 23)
    noise = jnp.clip(jax.random.normal(jax.random.fold_in(base, 1), (OBS, SLOTS, BS), jnp.float32), -6.0, 6.0)
    mixing = jax.random.normal(jax.random.fold_in(base, 3), (BS, BS), jnp.float32) / math.sqrt(BS)
    neighbour = jnp.roll(noise, -1, axis=1)
    coupled = noise + 0.35 * jnp.einsum('osx,xy->osy', neighbour, mixing)
    return jnp.clip(coupled, -80.0, 80.0)


def draw_blocks(key, part):
    return pick_blocks(key)


def draw_coefficients(key, part):
    return make_coefficients(key).astype(jnp.bfloat16)


def draw_residuals(key, part):
    coef = make_coefficients(key)
    chosen = pick_blocks(key)
    truth = jax.random.normal(jax.random.fold_in(key, 37), (G // BS, BS), jnp.float32)
    picked = truth[chosen]
    noise = jax.random.normal(jax.random.fold_in(key, 41), (OBS,), jnp.float32)
    values = jnp.sum(coef * picked, axis=(1, 2)) + noise
    return jnp.clip(values, -3000.0, 3000.0)


def setup_inputs(seed: int = 0) -> dict:
    key_list = jax.random.split(jax.random.key(seed), 4)
    blocks = draw_blocks(jax.random.fold_in(key_list[3], 71), 0)
    coefficients = draw_coefficients(jax.random.fold_in(key_list[3], 71), 0)
    residuals = draw_residuals(jax.random.fold_in(key_list[3], 71), 0)
    return {"blocks": blocks, "coefficients": coefficients, "residuals": residuals}


def reference(blocks, coefficients, residuals):
    total = blocks.shape[0]
    nblock = G // BS
    per_dev = nblock // N_GX
    group = math.gcd(total, 4096)
    count = total // group
    labels = jnp.arange(nblock, dtype=jnp.int32)

    def accumulate(carry, index):
        start = (index * group).astype(jnp.int32)
        picked = lax.dynamic_slice_in_dim(blocks, start, group, 0)
        coef = lax.dynamic_slice_in_dim(coefficients, start, group, 0).astype(jnp.float32)
        resid = lax.dynamic_slice_in_dim(residuals, start, group, 0)
        placed = (picked[:, :, None] == labels[None, None, :]).astype(jnp.float32)
        design = jnp.einsum('osa,osx->oax', placed, coef, precision=lax.Precision.HIGHEST).reshape(group, G)
        normal = carry[0] + jnp.dot(design.T.astype(jnp.float32), design.astype(jnp.float32), precision=lax.Precision.HIGHEST, preferred_element_type=jnp.float32)
        rhs = carry[1] + jnp.dot(resid.astype(jnp.float32), design.astype(jnp.float32), precision=lax.Precision.HIGHEST, preferred_element_type=jnp.float32)
        return ((normal, rhs), None)
    start_state = (jnp.zeros((G, G), jnp.float32), jnp.zeros((G,), jnp.float32))
    (normal, rhs), _ = lax.scan(accumulate, start_state, jnp.arange(count, dtype=jnp.int32))
    normal = normal / total
    rhs = rhs / total
    lower = jnp.linalg.cholesky(normal)
    middle = jax.scipy.linalg.solve_triangular(lower, rhs, lower=True)
    answer = jax.scipy.linalg.solve_triangular(lower.T, middle, lower=False)
    factor = lower.reshape(per_dev, N_GX, BS, per_dev, N_GY, BS).transpose(1, 0, 2, 4, 3, 5)
    return (factor, answer.reshape(nblock, BS))
```

```python
import functools

import jax
import jax.numpy as jnp
from jax import lax
from jax.experimental import pallas as pl
from jax.experimental.pallas import tpu as pltpu
from jax.sharding import PartitionSpec as P

G = 2048
BS = 128
SB = 2 * BS
NS = G // SB
EXTRA = 16
F32 = jnp.float32
BF16 = jnp.bfloat16
MESH = pl.DeviceIdType.MESH
TILES = [(i, j) for j in range(NS) for i in range(j, NS)]
ROWS = len(TILES) * SB
HALF = ROWS // 2
CHUNK = HALF // 3
ORDERS = ("xyz", "yzx", "zxy")


def gram_kernel(scale, blk_ref, coef_ref, res_ref, out_ref, design, flipped):
    obs = blk_ref.shape[0]
    slots = blk_ref.shape[1]
    step = 256

    def place(t, c):
        rows = pl.ds(pl.multiple_of(t * step, step), step)
        ids = [jnp.broadcast_to(blk_ref[rows, s : s + 1], (step, BS)) for s in range(slots)]
        vals = [coef_ref[rows, s * BS : (s + 1) * BS].astype(F32) for s in range(slots)]
        for b in range(G // BS):
            d = jnp.zeros((step, BS), F32)
            for s in range(slots):
                d = jnp.where(ids[s] == b, vals[s], d)
            db = d.astype(BF16)
            design[rows, b * BS : (b + 1) * BS] = db
            flipped[b * BS : (b + 1) * BS, rows] = db.T
        return c

    lax.fori_loop(0, obs // step, place, 0)

    res = res_ref[...]
    r1 = res.astype(BF16)
    rest = res - r1.astype(F32)
    r2 = rest.astype(BF16)
    r3 = (rest - r2.astype(F32)).astype(BF16)
    first = lax.broadcasted_iota(jnp.int32, (8, obs), 0)
    lhs = jnp.where(first == 0, r1.astype(F32), jnp.where(first == 1, r2.astype(F32), jnp.where(first == 2, r3.astype(F32), 0.0))).astype(BF16)

    for j in range(NS):
        base = TILES.index((j, j)) * SB
        cols = design[:, j * SB : (j + 1) * SB]

        def tile(i, c):
            rows = pl.ds(pl.multiple_of(i * SB, SB), SB)
            out = pl.ds(pl.multiple_of(base + (i - j) * SB, SB), SB)
            out_ref[out, :] = dot_nn(flipped[rows, :], cols) * scale
            return c

        lax.fori_loop(j, NS, tile, 0)
        side = jnp.sum(dot_nn(lhs, cols), axis=0, keepdims=True) * scale
        out_ref[base : base + 1, BS:] = side[:, :BS]
        out_ref[base + 1 : base + 2, BS:] = side[:, BS:]


def gram_call(blocks, coefficients, residuals, scale):
    obs = blocks.shape[0]
    return pl.pallas_call(
        functools.partial(gram_kernel, scale),
        out_shape=jax.ShapeDtypeStruct((ROWS, SB), F32),
        in_specs=[pl.BlockSpec(memory_space=pltpu.VMEM)] * 3,
        out_specs=pl.BlockSpec(memory_space=pltpu.VMEM),
        scratch_shapes=[pltpu.VMEM((obs, G), BF16), pltpu.VMEM((G, obs), BF16)],
        compiler_params=pltpu.CompilerParams(vmem_limit_bytes=60 * 1024 * 1024),
        name="gram",
    )(blocks, coefficients.reshape(obs, -1), residuals.reshape(1, obs))


def place_of(x, y, z, core):
    return (lax.rem(y, 2) * 4 + x, z * 2 + core, y // 2)


def reduce_kernel(in_ref, out_ref, work, near, far, core_sem, rs_sem, ag_sem, end_sem):
    gx, gy, gz = lax.axis_index("gx"), lax.axis_index("gy"), lax.axis_index("gz")
    at = {"x": lax.rem(gx, 4), "y": gz * 2 + gx // 4, "z": gy // 2}
    core = lax.rem(gy, 2)

    def device(axis=None, shift=0):
        c = dict(at)
        if axis is not None:
            c[axis] = lax.rem(c[axis] + shift + 4, 4)
        return place_of(c["x"], c["y"], c["z"], core)

    twin = place_of(at["x"], at["y"], at["z"], 1 - core)
    barrier = pltpu.get_barrier_semaphore()
    for axis in "xyz":
        for shift in (1, -1):
            pl.semaphore_signal(barrier, inc=1, device_id=device(axis, shift), device_id_type=MESH)
    pl.semaphore_signal(barrier, inc=1, device_id=twin, device_id_type=MESH)
    pl.semaphore_wait(barrier, 7)

    def remote(src, dst, sems, to):
        copy = pltpu.make_async_remote_copy(
            src_ref=src, dst_ref=dst, send_sem=sems.at[0], recv_sem=sems.at[1], device_id=to, device_id_type=MESH
        )
        copy.start()
        return copy

    mine = core * HALF
    other = (1 - core) * HALF
    pending = []

    def ds(start, size):
        return pl.ds(pl.multiple_of(start, 8), size)

    swaps = []
    for c in range(3):
        swaps.append(remote(in_ref.at[ds(other + c * CHUNK, CHUNK)], work.at[ds(c * CHUNK, CHUNK)], core_sem.at[c], twin))
    pending += swaps

    def add(dst, dst_start, src, src_start, size):
        step = 8 if size % 32 else 32

        def body(t, carry):
            d = ds(dst_start + t * step, step)
            dst[d, :] = dst[d, :] + src[ds(src_start + t * step, step), :]
            return carry

        lax.fori_loop(0, size // step, body, 0)

    bases = [c * CHUNK for c in range(3)]
    history = [[] for _ in range(3)]
    size = CHUNK
    offset = 0
    for p in range(3):
        unit = size // 4
        left = (unit // 2 + 7) // 8 * 8
        right = unit - left
        state = []
        for c in range(3):
            if p == 0:
                swaps[c].wait_recv()
                add(work, c * CHUNK, in_ref, mine + c * CHUNK, CHUNK)
            axis = ORDERS[c][p]
            m = at[axis]
            up, down = device(axis, 1), device(axis, -1)

            def piece(i, base=bases[c], m=m, unit=unit):
                return base + lax.rem(m + i + 4, 4) * unit

            half = near.at[c]
            a = remote(work.at[ds(piece(2), left)], half.at[ds(offset, left)], rs_sem.at[c, p, 0], up)
            b = remote(work.at[ds(piece(2) + left, right)], half.at[ds(offset + left, right)], rs_sem.at[c, p, 1], down)
            pending += [a, b]
            state.append((piece, up, down, a, b))
        ends = []
        for c in range(3):
            piece, up, down, a, b = state[c]
            a.wait_recv()
            add(work, piece(1), near.at[c], offset, left)
            u = remote(work.at[ds(piece(1), unit)], far.at[c, 0, ds(offset, unit)], rs_sem.at[c, p, 2], up)
            b.wait_recv()
            add(work, piece(-1) + left, near.at[c], offset + left, right)
            d = remote(work.at[ds(piece(-1), unit)], far.at[c, 1, ds(offset, unit)], rs_sem.at[c, p, 3], down)
            pending += [u, d]
            ends.append((u, d))
        for c in range(3):
            piece = state[c][0]
            for side in range(2):
                ends[c][side].wait_recv()
                add(work, piece(0), far.at[c, side], offset, unit)
            history[c].append((piece, state[c][1], state[c][2], unit, left, right))
            bases[c] = piece(0)
        offset += unit
        size = unit

    for c in range(3):
        unit = history[c][2][3]
        out_ref[ds(mine + bases[c], unit), :] = work[ds(bases[c], unit), :]
    for p in (2, 1, 0):
        firsts = []
        for c in range(3):
            piece, up, down, unit, left, right = history[c][p]
            own = out_ref.at[ds(mine + piece(0), unit)]
            u = remote(own, own, ag_sem.at[c, p, 0], up)
            d = remote(own, own, ag_sem.at[c, p, 1], down)
            pending += [u, d]
            firsts.append((u, d))
        seconds = []
        for c in range(3):
            piece, up, down, unit, left, right = history[c][p]
            firsts[c][0].wait_recv()
            part = out_ref.at[ds(mine + piece(-1), left)]
            u = remote(part, part, ag_sem.at[c, p, 2], up)
            firsts[c][1].wait_recv()
            part = out_ref.at[ds(mine + piece(1) + left, right)]
            d = remote(part, part, ag_sem.at[c, p, 3], down)
            pending += [u, d]
            seconds.append((u, d))
        for c in range(3):
            seconds[c][0].wait_recv()
            seconds[c][1].wait_recv()
    lasts = []
    for c in range(3):
        part = out_ref.at[ds(mine + c * CHUNK, CHUNK)]
        lasts.append(remote(part, part, end_sem.at[c], twin))
    for c in range(3):
        lasts[c].wait_recv()
    for copy in pending + lasts:
        copy.wait_send()


def reduce_call(payload):
    units = CHUNK // 4 + CHUNK // 16 + CHUNK // 64
    return pl.pallas_call(
        reduce_kernel,
        out_shape=jax.ShapeDtypeStruct((ROWS, SB), F32),
        in_specs=[pl.BlockSpec(memory_space=pltpu.VMEM)],
        out_specs=pl.BlockSpec(memory_space=pltpu.VMEM),
        scratch_shapes=[
            pltpu.VMEM((HALF, SB), F32),
            pltpu.VMEM((3, units, SB), F32),
            pltpu.VMEM((3, 2, units, SB), F32),
            pltpu.SemaphoreType.DMA((3, 2)),
            pltpu.SemaphoreType.DMA((3, 3, 4, 2)),
            pltpu.SemaphoreType.DMA((3, 3, 4, 2)),
            pltpu.SemaphoreType.DMA((3, 2)),
        ],
        compiler_params=pltpu.CompilerParams(
            vmem_limit_bytes=60 * 1024 * 1024, collective_id=0, has_side_effects=True
        ),
        name="reduce",
    )(payload)


def split(x):
    hi = x.astype(BF16)
    return hi, (x - hi.astype(F32)).astype(BF16)


def dot_nt(a, b):
    return lax.dot_general(a, b, (((1,), (1,)), ((), ())), preferred_element_type=F32)


def dot_nn(a, b):
    return lax.dot_general(a, b, (((1,), (0,)), ((), ())), preferred_element_type=F32)


def lane_all(x, lane):
    return jnp.broadcast_to(x[:, lane : lane + 1], x.shape)


def row_all(x, row):
    return jnp.broadcast_to(x[row : row + 1, :], x.shape)


def eliminate(w):
    lane = lax.broadcasted_iota(jnp.int32, (8, BS), 1)
    sub = lax.broadcasted_iota(jnp.int32, (8, BS), 0)
    w = list(w)
    for g in range(len(w)):
        r = w[g]
        cols = [lane_all(r, 8 * g + j) for j in range(8)]
        roots, rows, upper = [], [], []
        for j in range(8):
            root = lax.rsqrt(row_all(cols[j], j))
            below = jnp.where(sub > j, cols[j] * root, 0.0)
            here = lane == 8 * g + j
            row = row_all(jnp.where(here, 1.0, r), j) * root
            r = jnp.where(sub == j, row, jnp.where(here & (sub > j), 0.0, r) - below * row)
            ups = {}
            for l in range(j + 1, 8):
                ups[l] = row_all(cols[l], j) * root
                cols[l] = cols[l] - below * ups[l]
            roots.append(root)
            rows.append(jnp.where((lane > 8 * g + j) & (lane < 8 * g + 8), 0.0, row))
            upper.append(ups)
        w[g] = r
        group = (lane >= 8 * g) & (lane < 8 * g + 8)
        for i in range(g + 1, len(w)):
            c = [lane_all(w[i], 8 * g + j) for j in range(8)]
            acc = jnp.where(group, 0.0, w[i])
            for j in range(8):
                m = c[j] * roots[j]
                for l in range(j + 1, 8):
                    c[l] = c[l] - m * upper[j][l]
                acc = acc - m * rows[j]
            w[i] = acc
    return w


def chol_kernel(pos_ref, mat_ref, out_ref, sol_ref, a_ref, hi_ref, lo_ref, inv_ref, sem):
    n = G // BS
    copies = []
    for t, (i, j) in enumerate(TILES):
        copies.append(
            pltpu.make_async_copy(
                mat_ref.at[pl.ds(t * SB, SB)], a_ref.at[pl.ds(i * SB, SB), pl.ds(j * SB, SB)], sem.at[t]
            )
        )
        copies[-1].start()
    a_ref[pl.ds(G, EXTRA), :] = jnp.zeros((EXTRA, G), F32)
    for copy in copies:
        copy.wait()
    for j in range(NS):
        for h in range(2):
            a_ref[G : G + 1, j * SB + h * BS : j * SB + (h + 1) * BS] = a_ref[j * SB + h : j * SB + h + 1, j * SB + BS : (j + 1) * SB]
    lane2 = lax.broadcasted_iota(jnp.int32, (BS, BS), 1)
    sub2 = lax.broadcasted_iota(jnp.int32, (BS, BS), 0)

    def step(k, carry):
        at = pl.multiple_of(k * BS, BS)
        cols = pl.ds(at, BS)
        block = a_ref[pl.ds(at, BS), cols]
        w = eliminate([block[8 * i : 8 * i + 8] for i in range(BS // 8)])
        w = jnp.concatenate(w, axis=0)
        inv = jnp.where(lane2 <= sub2, w, 0.0)
        inv_ref[pl.ds(at, BS), :] = inv
        ih, il = split(inv)
        both = jnp.concatenate([ih, il], axis=0)
        diag = jnp.where(lane2 == sub2, 1.0 / w, jnp.where(lane2 > sub2, w, 0.0)).T
        a_ref[pl.ds(at, BS), cols] = diag
        dh, dl = split(diag)
        hi_ref[pl.ds(at, BS), cols] = dh
        lo_ref[pl.ds(at, BS), cols] = dl

        def solve(start, size):
            rows = pl.ds(start, size)
            xh, xl = split(a_ref[rows, cols])
            o = dot_nt(xh, both)
            o = o[:, :BS] + o[:, BS:] + dot_nt(xl, ih)
            a_ref[rows, cols] = o
            oh, ol = split(o)
            hi_ref[rows, cols] = oh
            lo_ref[rows, cols] = ol

        solve(G, EXTRA)
        odd = k % 2

        @pl.when(odd == 0)
        def _():
            solve(pl.multiple_of(at + BS, BS), BS)

        def solve_tile(t, c):
            solve(pl.multiple_of(t * 2 * BS, 2 * BS), 2 * BS)
            return c

        lax.fori_loop(k // 2 + 1, n // 2, solve_tile, 0)

        @pl.when(odd == 0)
        def _():
            nxt = pl.multiple_of(at + BS, BS)
            ncols = pl.ds(nxt, BS)
            bh = hi_ref[pl.ds(nxt, BS), cols]
            bl = lo_ref[pl.ds(nxt, BS), cols]
            bb = jnp.concatenate([bh, bl], axis=0)

            def update(start, size):
                rows = pl.ds(start, size)
                o = dot_nt(hi_ref[rows, cols], bb)
                o = o[:, :BS] + o[:, BS:] + dot_nt(lo_ref[rows, cols], bh)
                a_ref[rows, ncols] = a_ref[rows, ncols] - o

            update(G, EXTRA)
            update(nxt, BS)

            def tile(t, c):
                update(pl.multiple_of(t * 2 * BS, 2 * BS), 2 * BS)
                return c

            lax.fori_loop(k // 2 + 1, n // 2, tile, 0)

        @pl.when(odd == 1)
        def _():
            kk = k // 2
            pc = pl.ds(pl.multiple_of(kk * 2 * BS, 2 * BS), 2 * BS)

            def outer(jj, c):
                jc = pl.ds(pl.multiple_of(jj * 2 * BS, 2 * BS), 2 * BS)
                rh = hi_ref[jc, pc]
                rl = lo_ref[jc, pc]

                def update(rows):
                    xh = hi_ref[rows, pc]
                    xl = lo_ref[rows, pc]
                    o = dot_nt(xh, rh) + dot_nt(xl, rh) + dot_nt(xh, rl)
                    a_ref[rows, jc] = a_ref[rows, jc] - o

                update(pl.ds(G, EXTRA))

                def inner(ii, c2):
                    update(pl.ds(pl.multiple_of(ii * 2 * BS, 2 * BS), 2 * BS))
                    return c2

                lax.fori_loop(jj, n // 2, inner, 0)
                return c

            lax.fori_loop(kk + 1, n // 2, outer, 0)

        return carry

    lax.fori_loop(0, n, step, 0)

    def back(s, c):
        k = n - 1 - s
        at = pl.multiple_of(k * BS, BS)
        cols = pl.ds(at, BS)
        ih, il = split(inv_ref[pl.ds(at, BS), :])
        yh, yl = split(a_ref[pl.ds(G, EXTRA), cols])
        z = dot_nn(yh, ih) + dot_nn(yl, ih) + dot_nn(yh, il)
        sol_ref[:, cols] = z[:8]
        zh, zl = split(z)

        def sub(j, c2):
            jc = pl.ds(pl.multiple_of(j * BS, BS), BS)
            lh = hi_ref[pl.ds(at, BS), jc]
            ll = lo_ref[pl.ds(at, BS), jc]
            a_ref[pl.ds(G, EXTRA), jc] = a_ref[pl.ds(G, EXTRA), jc] - (dot_nn(zh, lh) + dot_nn(zl, lh) + dot_nn(zh, ll))
            return c2

        lax.fori_loop(0, k, sub, 0)
        return c

    lax.fori_loop(0, n, back, 0)

    p, q = pos_ref[0], pos_ref[1]
    for r in range(2):
        for c in range(2):
            rb = r * 8 + p
            cb = c * 8 + q
            blk = a_ref[pl.ds(pl.multiple_of(rb * BS, BS), BS), pl.ds(pl.multiple_of(cb * BS, BS), BS)]
            out_ref[r, :, c * BS : (c + 1) * BS] = jnp.where(rb >= cb, blk, 0.0)


def cholesky_call(pos, payload):
    return pl.pallas_call(
        chol_kernel,
        out_shape=(jax.ShapeDtypeStruct((2, BS, 2 * BS), F32), jax.ShapeDtypeStruct((8, G), F32)),
        in_specs=[
            pl.BlockSpec(memory_space=pltpu.SMEM),
            pl.BlockSpec(memory_space=pl.ANY),
        ],
        out_specs=(pl.BlockSpec(memory_space=pltpu.VMEM), pl.BlockSpec(memory_space=pltpu.VMEM)),
        scratch_shapes=[
            pltpu.VMEM((G + EXTRA, G), F32),
            pltpu.VMEM((G + EXTRA, G), BF16),
            pltpu.VMEM((G + EXTRA, G), BF16),
            pltpu.VMEM((G, BS), F32),
            pltpu.SemaphoreType.DMA((len(TILES),)),
        ],
        compiler_params=pltpu.CompilerParams(vmem_limit_bytes=60 * 1024 * 1024),
        name="chol",
    )(pos, payload)


def on_device(total, blocks, coefficients, residuals):
    payload = gram_call(blocks, coefficients, residuals, 1.0 / total)
    payload = reduce_call(payload)
    pos = jnp.stack([lax.axis_index("gx"), lax.axis_index("gy")]).astype(jnp.int32)
    factor, answer = cholesky_call(pos, payload)
    return factor.reshape(1, 2, BS, 1, 2, BS), answer[0].reshape(G // BS, BS)


def solution(mesh):
    def whole(blocks, coefficients, residuals):
        spread = P(("gx", "gy", "gz"))
        return jax.shard_map(
            functools.partial(on_device, blocks.shape[0]),
            mesh=mesh,
            in_specs=(spread, spread, spread),
            out_specs=(P("gx", None, None, "gy", None, None), P()),
            check_vma=False,
        )(blocks, coefficients, residuals)

    return whole
```

```python
import functools

import jax
import jax.numpy as jnp
from jax import lax
from jax.experimental import pallas as pl
from jax.experimental.pallas import tpu as pltpu
from jax.sharding import PartitionSpec as P

G = 2048
BS = 128
SB = 2 * BS
NS = G // SB
EXTRA = 16
F32 = jnp.float32
BF16 = jnp.bfloat16
MESH = pl.DeviceIdType.MESH
TILES = [(i, j) for j in range(NS) for i in range(j, NS)]
ROWS = len(TILES) * SB
HALF = ROWS // 2
CHUNK = HALF // 3
ORDERS = ("xyz", "yzx", "zxy")


def gram_kernel(scale, blk_ref, coef_ref, res_ref, out_ref, design, flipped):
    obs = blk_ref.shape[0]
    slots = blk_ref.shape[1]
    step = 256

    def place(t, c):
        rows = pl.ds(pl.multiple_of(t * step, step), step)
        ids = [jnp.broadcast_to(blk_ref[rows, s : s + 1], (step, BS)) for s in range(slots)]
        vals = [coef_ref[rows, s * BS : (s + 1) * BS].astype(F32) for s in range(slots)]
        for b in range(G // BS):
            d = jnp.zeros((step, BS), F32)
            for s in range(slots):
                d = jnp.where(ids[s] == b, vals[s], d)
            db = d.astype(BF16)
            design[rows, b * BS : (b + 1) * BS] = db
            flipped[b * BS : (b + 1) * BS, rows] = db.T
        return c

    lax.fori_loop(0, obs // step, place, 0)

    res = res_ref[...]
    r1 = res.astype(BF16)
    rest = res - r1.astype(F32)
    r2 = rest.astype(BF16)
    r3 = (rest - r2.astype(F32)).astype(BF16)
    first = lax.broadcasted_iota(jnp.int32, (8, obs), 0)
    lhs = jnp.where(first == 0, r1.astype(F32), jnp.where(first == 1, r2.astype(F32), jnp.where(first == 2, r3.astype(F32), 0.0))).astype(BF16)

    for j in range(NS):
        base = TILES.index((j, j)) * SB
        cols = design[:, j * SB : (j + 1) * SB]

        def tile(i, c):
            rows = pl.ds(pl.multiple_of(i * SB, SB), SB)
            out = pl.ds(pl.multiple_of(base + (i - j) * SB, SB), SB)
            out_ref[out, :] = dot_nn(flipped[rows, :], cols) * scale
            return c

        lax.fori_loop(j, NS, tile, 0)
        side = jnp.sum(dot_nn(lhs, cols), axis=0, keepdims=True) * scale
        out_ref[base : base + 1, BS:] = side[:, :BS]
        out_ref[base + 1 : base + 2, BS:] = side[:, BS:]


def gram_call(blocks, coefficients, residuals, scale):
    obs = blocks.shape[0]
    return pl.pallas_call(
        functools.partial(gram_kernel, scale),
        out_shape=jax.ShapeDtypeStruct((ROWS, SB), F32),
        in_specs=[pl.BlockSpec(memory_space=pltpu.VMEM)] * 3,
        out_specs=pl.BlockSpec(memory_space=pltpu.VMEM),
        scratch_shapes=[pltpu.VMEM((obs, G), BF16), pltpu.VMEM((G, obs), BF16)],
        compiler_params=pltpu.CompilerParams(vmem_limit_bytes=60 * 1024 * 1024),
        name="gram",
    )(blocks, coefficients.reshape(obs, -1), residuals.reshape(1, obs))


def place_of(x, y, z, core):
    return (lax.rem(y, 2) * 4 + x, z * 2 + core, y // 2)


def reduce_kernel(in_ref, out_ref, work, near, far, core_sem, rs_sem, ag_sem, end_sem):
    gx, gy, gz = lax.axis_index("gx"), lax.axis_index("gy"), lax.axis_index("gz")
    at = {"x": lax.rem(gx, 4), "y": gz * 2 + gx // 4, "z": gy // 2}
    core = lax.rem(gy, 2)

    def device(axis=None, shift=0):
        c = dict(at)
        if axis is not None:
            c[axis] = lax.rem(c[axis] + shift + 4, 4)
        return place_of(c["x"], c["y"], c["z"], core)

    twin = place_of(at["x"], at["y"], at["z"], 1 - core)
    barrier = pltpu.get_barrier_semaphore()
    for axis in "xyz":
        for shift in (1, -1):
            pl.semaphore_signal(barrier, inc=1, device_id=device(axis, shift), device_id_type=MESH)
    pl.semaphore_signal(barrier, inc=1, device_id=twin, device_id_type=MESH)
    pl.semaphore_wait(barrier, 7)

    def remote(src, dst, sems, to):
        copy = pltpu.make_async_remote_copy(
            src_ref=src, dst_ref=dst, send_sem=sems.at[0], recv_sem=sems.at[1], device_id=to, device_id_type=MESH
        )
        copy.start()
        return copy

    mine = core * HALF
    other = (1 - core) * HALF
    pending = []

    def ds(start, size):
        return pl.ds(pl.multiple_of(start, 8), size)

    swaps = []
    for c in range(3):
        swaps.append(remote(in_ref.at[ds(other + c * CHUNK, CHUNK)], work.at[ds(c * CHUNK, CHUNK)], core_sem.at[c], twin))
    pending += swaps

    def add(dst, dst_start, src, src_start, size):
        step = 8 if size % 32 else 32

        def body(t, carry):
            d = ds(dst_start + t * step, step)
            dst[d, :] = dst[d, :] + src[ds(src_start + t * step, step), :]
            return carry

        lax.fori_loop(0, size // step, body, 0)

    bases = [c * CHUNK for c in range(3)]
    history = [[] for _ in range(3)]
    size = CHUNK
    offset = 0
    for p in range(3):
        unit = size // 4
        left = (unit // 2 + 7) // 8 * 8
        right = unit - left
        state = []
        for c in range(3):
            if p == 0:
                swaps[c].wait_recv()
                add(work, c * CHUNK, in_ref, mine + c * CHUNK, CHUNK)
            axis = ORDERS[c][p]
            m = at[axis]
            up, down = device(axis, 1), device(axis, -1)

            def piece(i, base=bases[c], m=m, unit=unit):
                return base + lax.rem(m + i + 4, 4) * unit

            half = near.at[c]
            a = remote(work.at[ds(piece(2), left)], half.at[ds(offset, left)], rs_sem.at[c, p, 0], up)
            b = remote(work.at[ds(piece(2) + left, right)], half.at[ds(offset + left, right)], rs_sem.at[c, p, 1], down)
            pending += [a, b]
            state.append((piece, up, down, a, b))
        ends = []
        for c in range(3):
            piece, up, down, a, b = state[c]
            a.wait_recv()
            add(work, piece(1), near.at[c], offset, left)
            u = remote(work.at[ds(piece(1), unit)], far.at[c, 0, ds(offset, unit)], rs_sem.at[c, p, 2], up)
            b.wait_recv()
            add(work, piece(-1) + left, near.at[c], offset + left, right)
            d = remote(work.at[ds(piece(-1), unit)], far.at[c, 1, ds(offset, unit)], rs_sem.at[c, p, 3], down)
            pending += [u, d]
            ends.append((u, d))
        for c in range(3):
            piece = state[c][0]
            for side in range(2):
                ends[c][side].wait_recv()
                add(work, piece(0), far.at[c, side], offset, unit)
            history[c].append((piece, state[c][1], state[c][2], unit, left, right))
            bases[c] = piece(0)
        offset += unit
        size = unit

    for c in range(3):
        unit = history[c][2][3]
        out_ref[ds(mine + bases[c], unit), :] = work[ds(bases[c], unit), :]
    for p in (2, 1, 0):
        firsts = []
        for c in range(3):
            piece, up, down, unit, left, right = history[c][p]
            own = out_ref.at[ds(mine + piece(0), unit)]
            u = remote(own, own, ag_sem.at[c, p, 0], up)
            d = remote(own, own, ag_sem.at[c, p, 1], down)
            pending += [u, d]
            firsts.append((u, d))
        seconds = []
        for c in range(3):
            piece, up, down, unit, left, right = history[c][p]
            firsts[c][0].wait_recv()
            part = out_ref.at[ds(mine + piece(-1), left)]
            u = remote(part, part, ag_sem.at[c, p, 2], up)
            firsts[c][1].wait_recv()
            part = out_ref.at[ds(mine + piece(1) + left, right)]
            d = remote(part, part, ag_sem.at[c, p, 3], down)
            pending += [u, d]
            seconds.append((u, d))
        for c in range(3):
            seconds[c][0].wait_recv()
            seconds[c][1].wait_recv()
    lasts = []
    for c in range(3):
        part = out_ref.at[ds(mine + c * CHUNK, CHUNK)]
        lasts.append(remote(part, part, end_sem.at[c], twin))
    for c in range(3):
        lasts[c].wait_recv()
    for copy in pending + lasts:
        copy.wait_send()


def reduce_call(payload):
    units = CHUNK // 4 + CHUNK // 16 + CHUNK // 64
    return pl.pallas_call(
        reduce_kernel,
        out_shape=jax.ShapeDtypeStruct((ROWS, SB), F32),
        in_specs=[pl.BlockSpec(memory_space=pltpu.VMEM)],
        out_specs=pl.BlockSpec(memory_space=pltpu.VMEM),
        scratch_shapes=[
            pltpu.VMEM((HALF, SB), F32),
            pltpu.VMEM((3, units, SB), F32),
            pltpu.VMEM((3, 2, units, SB), F32),
            pltpu.SemaphoreType.DMA((3, 2)),
            pltpu.SemaphoreType.DMA((3, 3, 4, 2)),
            pltpu.SemaphoreType.DMA((3, 3, 4, 2)),
            pltpu.SemaphoreType.DMA((3, 2)),
        ],
        compiler_params=pltpu.CompilerParams(
            vmem_limit_bytes=60 * 1024 * 1024, collective_id=0, has_side_effects=True
        ),
        name="reduce",
    )(payload)


def split(x):
    hi = x.astype(BF16)
    return hi, (x - hi.astype(F32)).astype(BF16)


def dot_nt(a, b):
    return lax.dot_general(a, b, (((1,), (1,)), ((), ())), preferred_element_type=F32)


def dot_nn(a, b):
    return lax.dot_general(a, b, (((1,), (0,)), ((), ())), preferred_element_type=F32)


def lane_all(x, lane):
    return jnp.broadcast_to(x[:, lane : lane + 1], x.shape)


def row_all(x, row):
    return jnp.broadcast_to(x[row : row + 1, :], x.shape)


NEAR = 3
DUMMY = G + EXTRA
TALL = DUMMY + SB + EXTRA
UNITS = 7
SIDES = NS - 1


def plan():
    n = 2 * NS
    sides = [[DUMMY] * SIDES for _ in range(n)]
    units = [[(DUMMY, 0, 0, 0)] * UNITS for _ in range(n)]
    todo = []
    for k in range(n):
        if k:
            first = (k - 1) // 2 + (1 if k % 2 else 2)
            for t, i in enumerate(range(first, NS)):
                sides[k][t] = i * SB
        if k >= 2 and k % 2 == 0:
            p = k // 2 - 1
            for j in range(p + 1, NS):
                for i in range(j, NS):
                    if (i, j) != (p + 1, p + 1):
                        todo.append((2 * j if i > j else 2 * j - 1, j, p, i))
        todo.sort()
        now, todo = todo[:UNITS], todo[UNITS:]
        for t, (limit, j, p, i) in enumerate(now):
            assert limit >= k
            units[k][t] = (i * SB, j * SB, p * SB, 1 if i == j else 0)
    assert not todo
    flat = []
    for k in range(n):
        flat.append(sides[k] + [v for u in units[k] for v in u])
    return flat


def eliminate(w, fill):
    lane = lax.broadcasted_iota(jnp.int32, (8, BS), 1)
    sub = lax.broadcasted_iota(jnp.int32, (8, BS), 0)
    w = list(w)
    count = len(w)
    cols = [lane_all(w[0], j) for j in range(8)]
    for g in range(count):
        r = w[g]
        group = (lane >= 8 * g) & (lane < 8 * g + 8)
        near = range(g + 1, min(g + 1 + NEAR, count))
        raw = {i: [lane_all(w[i], 8 * g + j) for j in range(8)] for i in near}
        ahead = [lane_all(w[g + 1], 8 * g + 8 + j) for j in range(8)] if g + 1 < count else None
        accs = {i: jnp.where(group, 0.0, w[i]) for i in near}
        for j in range(8):
            root = lax.rsqrt(row_all(cols[j], j))
            below = jnp.where(sub > j, cols[j] * root, 0.0)
            here = lane == 8 * g + j
            row = row_all(jnp.where(here, 1.0, r), j) * root
            r = jnp.where(sub == j, row, jnp.where(here & (sub > j), 0.0, r) - below * row)
            ups = {}
            for l in range(j + 1, 8):
                ups[l] = row_all(cols[l], j) * root
                cols[l] = cols[l] - below * ups[l]
            inverse_row = jnp.where((lane > 8 * g + j) & (lane < 8 * g + 8), 0.0, row)
            for i in near:
                c = raw[i]
                m = c[j] * root
                for l in range(j + 1, 8):
                    c[l] = c[l] - m * ups[l]
                accs[i] = accs[i] - m * inverse_row
                if i == g + 1:
                    ahead = [ahead[l] - m * row_all(m, l) for l in range(8)]
        w[g] = r
        for i in near:
            w[i] = accs[i]
        far = g + 1 + NEAR
        if far < count:
            x = jnp.where(lane >= 8 * far, r, 0.0)
            y = jnp.where(group & (lane > 8 * g + sub), 0.0, r)
            xh = x.astype(BF16).astype(F32)
            yh = y.astype(BF16).astype(F32)
            zero = jnp.zeros_like(x)
            xs = jnp.concatenate([xh, x - xh, xh, zero], axis=0).astype(BF16)
            ys = jnp.concatenate([yh, yh, y - yh, zero], axis=0).astype(BF16)
            delta = lax.dot_general(xs, ys, (((0,), (0,)), ((), ())), preferred_element_type=F32)
            for i in range(far, count):
                w[i] = jnp.where(group, 0.0, w[i]) - delta[8 * i : 8 * i + 8]
        cols = ahead
        fill(g)
    return w


def aligned(x, m=16):
    return pl.multiple_of(x, m)


def stacked(hi, lo):
    return jnp.concatenate(
        [jnp.concatenate([hi, hi], axis=1), jnp.concatenate([lo, jnp.zeros_like(lo)], axis=1)], axis=0
    )


def fold(o):
    return o[:, :BS] + o[:, BS:]


def chol_kernel(pos_ref, plan_ref, mat_ref, out_ref, sol_ref, a_ref, hi_ref, lo_ref, inv_ref, winv_ref, wnext_ref, sem):
    n = G // BS
    copies = []
    for t, (i, j) in enumerate(TILES):
        copies.append(
            pltpu.make_async_copy(
                mat_ref.at[pl.ds(t * SB, SB)], a_ref.at[pl.ds(i * SB, SB), pl.ds(j * SB, SB)], sem.at[t]
            )
        )
        copies[-1].start()
    a_ref[pl.ds(G, EXTRA), :] = jnp.zeros((EXTRA, G), F32)
    for copy in copies:
        copy.wait()
    for j in range(NS):
        for h in range(2):
            a_ref[G : G + 1, j * SB + h * BS : j * SB + (h + 1) * BS] = a_ref[
                j * SB + h : j * SB + h + 1, j * SB + BS : (j + 1) * SB
            ]
    lane2 = lax.broadcasted_iota(jnp.int32, (BS, BS), 1)
    sub2 = lax.broadcasted_iota(jnp.int32, (BS, BS), 0)
    ext = pl.ds(G, EXTRA)

    def put(rows, cols, o):
        oh, ol = split(o)
        a_ref[rows, cols] = o
        hi_ref[rows, cols] = oh
        lo_ref[rows, cols] = ol
        return jnp.concatenate([oh, ol], axis=1)

    def solved(rows_list, cols):
        x = jnp.concatenate([a_ref[rows, cols] for rows in rows_list], axis=0)
        xh, xl = split(x)
        return fold(dot_nt(jnp.concatenate([xh, xl], axis=1), winv_ref[...]))

    def update(rows, erows, jc, pc):
        xh = jnp.concatenate([hi_ref[rows, pc], hi_ref[ext, pc]], axis=0)
        xl = jnp.concatenate([lo_ref[rows, pc], lo_ref[ext, pc]], axis=0)
        rh, rl = hi_ref[jc, pc], lo_ref[jc, pc]
        o = dot_nt(xh, rh) + dot_nt(xl, rh) + dot_nt(xh, rl)
        a_ref[rows, jc] = a_ref[rows, jc] - o[:SB]
        a_ref[erows, jc] = a_ref[erows, jc] - o[SB:]

    def step(k, carry):
        at = aligned(k * BS, BS)
        cols = pl.ds(at, BS)
        odd = lax.rem(k, 2)
        prev = pl.ds(aligned(jnp.maximum(k - 1, 0) * BS, BS), BS)
        edummy = DUMMY + SB
        eside = pl.ds(aligned(jnp.where(odd == 1, G, edummy)), EXTRA)

        def fill(g):
            if g < SIDES:
                base = plan_ref[k, g]
                rows = pl.ds(aligned(base), SB)
                o = solved([rows, eside] if g == 0 else [rows], prev)
                both = put(rows, prev, o[:SB])
                if g == 0:
                    both = jnp.concatenate([both, put(eside, prev, o[SB:])], axis=0)
                d = fold(dot_nt(both, wnext_ref[...]))
                drows = pl.ds(aligned(jnp.where(odd == 1, base, DUMMY)), SB)
                a_ref[drows, cols] = a_ref[drows, cols] - d[:SB]
                if g == 0:
                    a_ref[eside, cols] = a_ref[eside, cols] - d[SB:]
            elif g < SIDES + UNITS:
                u = SIDES + 4 * (g - SIDES)
                rows = pl.ds(aligned(plan_ref[k, u]), SB)
                jc = pl.ds(aligned(plan_ref[k, u + 1], SB), SB)
                pc = pl.ds(aligned(plan_ref[k, u + 2], SB), SB)
                update(rows, pl.ds(aligned(jnp.where(plan_ref[k, u + 3] == 1, G, edummy)), EXTRA), jc, pc)

        block = a_ref[pl.ds(at, BS), cols]
        w = eliminate([block[8 * i : 8 * i + 8] for i in range(BS // 8)], fill)
        w = jnp.concatenate(w, axis=0)
        inv = jnp.where(lane2 <= sub2, w, 0.0)
        inv_ref[pl.ds(at, BS), :] = inv
        ih, il = split(inv)
        winv_ref[...] = stacked(ih, il)

        @pl.when(odd == 0)
        def _():
            nxt = pl.ds(aligned(at + BS, BS), BS)
            o = solved([nxt], cols)
            both = put(nxt, cols, o)
            weights = stacked(both[:, :BS], both[:, BS:])
            wnext_ref[...] = weights
            a_ref[nxt, nxt] = a_ref[nxt, nxt] - fold(dot_nt(both, weights))

        @pl.when((odd == 1) & (k < n - 1))
        def _():
            nxt = pl.ds(aligned(at + BS, BS), SB)
            o = solved([nxt, ext], cols)
            put(nxt, cols, o[:SB])
            put(ext, cols, o[SB:])
            update(nxt, ext, nxt, pl.ds(aligned(at - BS, SB), SB))

        @pl.when(k == n - 1)
        def _():
            put(ext, cols, solved([ext], cols))

        put(pl.ds(at, BS), cols, jnp.where(lane2 == sub2, 1.0 / w, jnp.where(lane2 > sub2, w, 0.0)).T)
        return carry

    lax.fori_loop(0, n, step, 0)

    def back(s, c):
        k = n - 1 - s
        at = aligned(k * BS, BS)
        cols = pl.ds(at, BS)
        ih, il = split(inv_ref[pl.ds(at, BS), :])
        yh, yl = split(a_ref[pl.ds(G, 8), cols])
        y = jnp.concatenate([yh, yl], axis=0)
        z = dot_nn(y, ih)
        z = z[:8] + z[8:] + dot_nn(yh, il)
        sol_ref[:, cols] = z
        zh, zl = split(z)
        zz = jnp.concatenate([zh, zl], axis=0)
        wide = 4 * BS

        def sub(j, c2):
            jc = pl.ds(aligned(j * wide, wide), wide)
            o = dot_nn(zz, hi_ref[pl.ds(at, BS), jc])
            a_ref[pl.ds(G, 8), jc] = a_ref[pl.ds(G, 8), jc] - (o[:8] + o[8:] + dot_nn(zh, lo_ref[pl.ds(at, BS), jc]))
            return c2

        lax.fori_loop(0, (k + 3) // 4, sub, 0)
        return c

    lax.fori_loop(0, n, back, 0)

    p, q = pos_ref[0], pos_ref[1]
    for r in range(2):
        for c in range(2):
            rb = r * 8 + p
            cb = c * 8 + q
            blk = a_ref[pl.ds(aligned(rb * BS, BS), BS), pl.ds(aligned(cb * BS, BS), BS)]
            out_ref[r, :, c * BS : (c + 1) * BS] = jnp.where(rb >= cb, blk, 0.0)


def cholesky_call(pos, payload):
    return pl.pallas_call(
        chol_kernel,
        out_shape=(jax.ShapeDtypeStruct((2, BS, 2 * BS), F32), jax.ShapeDtypeStruct((8, G), F32)),
        in_specs=[
            pl.BlockSpec(memory_space=pltpu.SMEM),
            pl.BlockSpec(memory_space=pltpu.SMEM),
            pl.BlockSpec(memory_space=pl.ANY),
        ],
        out_specs=(pl.BlockSpec(memory_space=pltpu.VMEM), pl.BlockSpec(memory_space=pltpu.VMEM)),
        scratch_shapes=[
            pltpu.VMEM((TALL, G), F32),
            pltpu.VMEM((TALL, G), BF16),
            pltpu.VMEM((TALL, G), BF16),
            pltpu.VMEM((G, BS), F32),
            pltpu.VMEM((SB, SB), BF16),
            pltpu.VMEM((SB, SB), BF16),
            pltpu.SemaphoreType.DMA((len(TILES),)),
        ],
        compiler_params=pltpu.CompilerParams(vmem_limit_bytes=60 * 1024 * 1024),
        name="chol",
    )(pos, jnp.asarray(plan(), jnp.int32), payload)


def on_device(total, blocks, coefficients, residuals):
    payload = gram_call(blocks, coefficients, residuals, 1.0 / total)
    payload = reduce_call(payload)
    pos = jnp.stack([lax.axis_index("gx"), lax.axis_index("gy")]).astype(jnp.int32)
    factor, answer = cholesky_call(pos, payload)
    return factor.reshape(1, 2, BS, 1, 2, BS), answer[0].reshape(G // BS, BS)


def solution(mesh):
    def whole(blocks, coefficients, residuals):
        spread = P(("gx", "gy", "gz"))
        return jax.shard_map(
            functools.partial(on_device, blocks.shape[0]),
            mesh=mesh,
            in_specs=(spread, spread, spread),
            out_specs=(P("gx", None, None, "gy", None, None), P()),
            check_vma=False,
        )(blocks, coefficients, residuals)

    return whole
```

```python
import functools

import jax
import jax.numpy as jnp
from jax import lax
from jax.experimental import pallas as pl
from jax.experimental.pallas import tpu as pltpu
from jax.sharding import PartitionSpec as P

G = 2048
BS = 128
SB = 2 * BS
NS = G // SB
EXTRA = 16
F32 = jnp.float32
BF16 = jnp.bfloat16
MESH = pl.DeviceIdType.MESH
ROUNDS = 3
STREAMS = 3 * ROUNDS
DIAG = [(j, j) for j in range(NS)]
SIDE = [(i, j) for j in range(NS) for i in range(j + 1, NS)]
TILES = DIAG[0::2] + SIDE[0::2] + DIAG[1::2] + SIDE[1::2]
ROWS = len(TILES) * SB
HALF = ROWS // 2
PART = HALF // STREAMS
UNITS_OF = (PART // 4, PART // 16, PART // 64)
ORDERS = ("xyz", "yzx", "zxy")


def split(x):
    hi = x.astype(BF16)
    return hi, (x - hi.astype(F32)).astype(BF16)


def dot_nt(a, b):
    return lax.dot_general(a, b, (((1,), (1,)), ((), ())), preferred_element_type=F32)


def dot_nn(a, b):
    return lax.dot_general(a, b, (((1,), (0,)), ((), ())), preferred_element_type=F32)


def lane_all(x, lane):
    return jnp.broadcast_to(x[:, lane : lane + 1], x.shape)


def row_all(x, row):
    return jnp.broadcast_to(x[row : row + 1, :], x.shape)


def place_of(x, y, z, core):
    return (lax.rem(y, 2) * 4 + x, z * 2 + core, y // 2)


def halves(unit):
    left = (unit // 2 + 7) // 8 * 8
    return left, unit - left


def reduce_kernel(scale, blk_ref, coef_ref, res_ref, pay, design, flipped, outbox, inbox, work, near, far, swap_sem, rs_sem, ag_sem, end_sem):
    gx, gy, gz = lax.axis_index("gx"), lax.axis_index("gy"), lax.axis_index("gz")
    at = {"x": lax.rem(gx, 4), "y": gz * 2 + gx // 4, "z": gy // 2}
    core = lax.rem(gy, 2)

    def device(axis, shift):
        c = dict(at)
        c[axis] = lax.rem(c[axis] + shift + 4, 4)
        return place_of(c["x"], c["y"], c["z"], core)

    twin = place_of(at["x"], at["y"], at["z"], 1 - core)
    barrier = pltpu.get_barrier_semaphore()
    for axis in "xyz":
        for shift in (1, -1):
            pl.semaphore_signal(barrier, inc=1, device_id=device(axis, shift), device_id_type=MESH)
    pl.semaphore_signal(barrier, inc=1, device_id=twin, device_id_type=MESH)

    obs = blk_ref.shape[0]
    slots = blk_ref.shape[1]
    step = 256

    def place(t, c):
        rows = pl.ds(pl.multiple_of(t * step, step), step)
        ids = [jnp.broadcast_to(blk_ref[rows, s : s + 1], (step, BS)) for s in range(slots)]
        vals = [coef_ref[rows, s * BS : (s + 1) * BS].astype(F32) for s in range(slots)]
        for b in range(G // BS):
            d = jnp.zeros((step, BS), F32)
            for s in range(slots):
                d = jnp.where(ids[s] == b, vals[s], d)
            db = d.astype(BF16)
            design[rows, b * BS : (b + 1) * BS] = db
            flipped[b * BS : (b + 1) * BS, rows] = db.T
        return c

    lax.fori_loop(0, obs // step, place, 0)

    res = res_ref[...]
    r1 = res.astype(BF16).astype(F32)
    r2 = (res - r1).astype(BF16).astype(F32)
    r3 = res - r1 - r2
    first = lax.broadcasted_iota(jnp.int32, (8, obs), 0)
    lhs = jnp.where(first == 0, r1, jnp.where(first == 1, r2, jnp.where(first == 2, r3, 0.0))).astype(BF16)

    def ds(start, size):
        return pl.ds(pl.multiple_of(start, 8), size)

    mine = core * HALF

    def gram(side, slot, dst):
        (i0, j0), (i1, j1) = TILES[slot], TILES[slot + len(TILES) // 2]
        i = (i0 + (i1 - i0) * side) * SB
        j = (j0 + (j1 - j0) * side) * SB
        cols = design[:, pl.ds(pl.multiple_of(j, SB), SB)]
        base = slot * SB
        dst[base : base + SB, :] = dot_nn(flipped[pl.ds(pl.multiple_of(i, SB), SB), :], cols) * scale
        if i0 == j0:
            row = jnp.sum(dot_nn(lhs, cols), axis=0, keepdims=True) * scale
            dst[base : base + 8, BS:] = jnp.concatenate([row[:, :BS], row[:, BS:], jnp.zeros((6, BS), F32)], axis=0)

    started = []

    def remote(src, dst, sems, to):
        copy = pltpu.make_async_remote_copy(
            src_ref=src, dst_ref=dst, send_sem=sems.at[0], recv_sem=sems.at[1], device_id=to, device_id_type=MESH
        )
        copy.start()
        started.append(copy)
        return copy

    def add(dst, dst_start, src, src_start, size):
        piece = min(size, 64)

        def body(t, carry):
            d = ds(dst_start + t * piece, piece)
            dst[d, :] = dst[d, :] + src[ds(src_start + t * piece, piece), :]
            return carry

        if size == piece:
            body(0, 0)
        else:
            lax.fori_loop(0, size // piece, body, 0)

    class Stream:
        def __init__(self, s):
            self.s = s
            self.order = ORDERS[s % 3]
            self.base = s * PART
            self.pieces = []

        def swap(self):
            rows = PART * self.s
            self.swapped = remote(outbox.at[ds(rows, PART)], inbox.at[ds(rows, PART)], swap_sem.at[self.s], twin)

        def opposite(self, p):
            s, unit = self.s, UNITS_OF[p]
            if p == 0:
                self.swapped.wait_recv()
                add(work, PART * s, inbox, PART * s, PART)
            else:
                self.finish(p - 1)
            axis = self.order[p]
            m, base = at[axis], self.base
            self.pieces.append(lambda i: base + lax.rem(m + i + 4, 4) * unit)
            left, right = halves(unit)
            piece, off = self.pieces[p], sum(UNITS_OF[:p])
            self.a = remote(work.at[ds(piece(2), left)], near.at[s, ds(off, left)], rs_sem.at[s, p, 0], device(axis, 1))
            if right:
                self.b = remote(
                    work.at[ds(piece(2) + left, right)], near.at[s, ds(off + left, right)], rs_sem.at[s, p, 1], device(axis, -1)
                )

        def sides(self, p):
            s, unit, axis, piece = self.s, UNITS_OF[p], self.order[p], self.pieces[p]
            left, right = halves(unit)
            off = sum(UNITS_OF[:p])
            self.a.wait_recv()
            add(work, piece(1), near.at[s], off, left)
            self.u = remote(work.at[ds(piece(1), unit)], far.at[s, 0, ds(off, unit)], rs_sem.at[s, p, 2], device(axis, 1))
            if right:
                self.b.wait_recv()
                add(work, piece(-1) + left, near.at[s], off + left, right)
            self.d = remote(work.at[ds(piece(-1), unit)], far.at[s, 1, ds(off, unit)], rs_sem.at[s, p, 3], device(axis, -1))

        def finish(self, p):
            s, unit, piece = self.s, UNITS_OF[p], self.pieces[p]
            off = sum(UNITS_OF[:p])
            for k, copy in enumerate((self.u, self.d)):
                copy.wait_recv()
                add(work, piece(0), far.at[s, k], off, unit)
            self.base = piece(0)

        def spread(self, p):
            s, unit, axis, piece = self.s, UNITS_OF[p], self.order[p], self.pieces[p]
            if p == 2:
                self.finish(2)
                pay[ds(mine + self.base, unit), :] = work[ds(self.base, unit), :]
            else:
                self.last.wait_recv()
                if self.last2 is not None:
                    self.last2.wait_recv()
            own = pay.at[ds(mine + piece(0), unit)]
            self.u = remote(own, own, ag_sem.at[s, p, 0], device(axis, 1))
            self.d = remote(own, own, ag_sem.at[s, p, 1], device(axis, -1))
            if p == 0:
                self.ends = [remote(own, own, end_sem.at[s, 0], twin)]

        def relay(self, p):
            s, unit, axis, piece = self.s, UNITS_OF[p], self.order[p], self.pieces[p]
            left, right = halves(unit)
            self.u.wait_recv()
            part = pay.at[ds(mine + piece(-1), left)]
            self.last = remote(part, part, ag_sem.at[s, p, 2], device(axis, 1))
            self.d.wait_recv()
            self.last2 = None
            if right:
                part = pay.at[ds(mine + piece(1) + left, right)]
                self.last2 = remote(part, part, ag_sem.at[s, p, 3], device(axis, -1))
            if p == 0:
                for k, i in ((1, -1), (2, 1)):
                    part = pay.at[ds(mine + piece(i), unit)]
                    self.ends.append(remote(part, part, end_sem.at[s, k], twin))

        def tail(self):
            self.last.wait_recv()
            if self.last2 is not None:
                self.last2.wait_recv()
            part = pay.at[ds(mine + self.pieces[0](2), UNITS_OF[0])]
            self.ends.append(remote(part, part, end_sem.at[self.s, 3], twin))

        def end(self):
            for copy in self.ends:
                copy.wait_recv()

        def run(self, stage):
            if stage < 6:
                (self.sides if stage % 2 else self.opposite)(stage // 2)
            elif stage < 12:
                (self.relay if stage % 2 else self.spread)(2 - (stage - 6) // 2)
            elif stage == 12:
                self.tail()
            elif stage == 13:
                self.end()

    streams = [Stream(s) for s in range(STREAMS)]
    per = PART // SB
    for t in range(14 + ROUNDS - 1):
        if t < ROUNDS:
            for s in range(3 * t, 3 * t + 3):
                for k in range(per):
                    gram(1 - core, s * per + k, outbox)
                if s == 0:
                    pl.semaphore_wait(barrier, 7)
                streams[s].swap()
            for s in range(3 * t, 3 * t + 3):
                for k in range(per):
                    gram(core, s * per + k, work)
        for r in range(ROUNDS):
            if 0 <= t - r < 14:
                for c in range(3):
                    streams[3 * r + c].run(t - r)
    for copy in started:
        copy.wait_send()


def reduce_call(blocks, coefficients, residuals, scale):
    obs = blocks.shape[0]
    units = sum(UNITS_OF)
    return pl.pallas_call(
        functools.partial(reduce_kernel, scale),
        out_shape=jax.ShapeDtypeStruct((ROWS, SB), F32),
        in_specs=[pl.BlockSpec(memory_space=pltpu.VMEM)] * 3,
        out_specs=pl.BlockSpec(memory_space=pltpu.VMEM),
        scratch_shapes=[
            pltpu.VMEM((obs, G), BF16),
            pltpu.VMEM((G, obs), BF16),
            pltpu.VMEM((HALF, SB), F32),
            pltpu.VMEM((HALF, SB), F32),
            pltpu.VMEM((HALF, SB), F32),
            pltpu.VMEM((STREAMS, units, SB), F32),
            pltpu.VMEM((STREAMS, 2, units, SB), F32),
            pltpu.SemaphoreType.DMA((STREAMS, 2)),
            pltpu.SemaphoreType.DMA((STREAMS, 3, 4, 2)),
            pltpu.SemaphoreType.DMA((STREAMS, 3, 4, 2)),
            pltpu.SemaphoreType.DMA((STREAMS, 4, 2)),
        ],
        compiler_params=pltpu.CompilerParams(
            vmem_limit_bytes=60 * 1024 * 1024, collective_id=0, has_side_effects=True
        ),
        name="reduce",
    )(blocks, coefficients.reshape(obs, -1), residuals.reshape(1, obs))


NEAR = 3
DUMMY = G + EXTRA
TALL = DUMMY + SB + EXTRA
UNITS = 7
SIDES = NS - 1


def plan():
    n = 2 * NS
    sides = [[DUMMY] * SIDES for _ in range(n)]
    units = [[(DUMMY, 0, 0, 0)] * UNITS for _ in range(n)]
    todo = []
    for k in range(n):
        if k:
            first = (k - 1) // 2 + (1 if k % 2 else 2)
            for t, i in enumerate(range(first, NS)):
                sides[k][t] = i * SB
        if k >= 2 and k % 2 == 0:
            p = k // 2 - 1
            for j in range(p + 1, NS):
                for i in range(j, NS):
                    if (i, j) != (p + 1, p + 1):
                        todo.append((2 * j if i > j else 2 * j - 1, j, p, i))
        todo.sort()
        now, todo = todo[:UNITS], todo[UNITS:]
        for t, (limit, j, p, i) in enumerate(now):
            assert limit >= k
            units[k][t] = (i * SB, j * SB, p * SB, 1 if i == j else 0)
    assert not todo
    flat = []
    for k in range(n):
        flat.append(sides[k] + [v for u in units[k] for v in u])
    return flat


def eliminate(w, fill):
    lane = lax.broadcasted_iota(jnp.int32, (8, BS), 1)
    sub = lax.broadcasted_iota(jnp.int32, (8, BS), 0)
    w = list(w)
    count = len(w)
    cols = [lane_all(w[0], j) for j in range(8)]
    for g in range(count):
        r = w[g]
        group = (lane >= 8 * g) & (lane < 8 * g + 8)
        near = range(g + 1, min(g + 1 + NEAR, count))
        raw = {i: [lane_all(w[i], 8 * g + j) for j in range(8)] for i in near}
        ahead = [lane_all(w[g + 1], 8 * g + 8 + j) for j in range(8)] if g + 1 < count else None
        accs = {i: jnp.where(group, 0.0, w[i]) for i in near}
        for j in range(8):
            root = lax.rsqrt(row_all(cols[j], j))
            below = jnp.where(sub > j, cols[j] * root, 0.0)
            here = lane == 8 * g + j
            row = row_all(jnp.where(here, 1.0, r), j) * root
            r = jnp.where(sub == j, row, jnp.where(here & (sub > j), 0.0, r) - below * row)
            ups = {}
            for l in range(j + 1, 8):
                ups[l] = row_all(cols[l], j) * root
                cols[l] = cols[l] - below * ups[l]
            inverse_row = jnp.where((lane > 8 * g + j) & (lane < 8 * g + 8), 0.0, row)
            for i in near:
                c = raw[i]
                m = c[j] * root
                for l in range(j + 1, 8):
                    c[l] = c[l] - m * ups[l]
                accs[i] = accs[i] - m * inverse_row
                if i == g + 1:
                    ahead = [ahead[l] - m * row_all(m, l) for l in range(8)]
        w[g] = r
        for i in near:
            w[i] = accs[i]
        far = g + 1 + NEAR
        if far < count:
            x = jnp.where(lane >= 8 * far, r, 0.0)
            y = jnp.where(group & (lane > 8 * g + sub), 0.0, r)
            xh = x.astype(BF16).astype(F32)
            yh = y.astype(BF16).astype(F32)
            zero = jnp.zeros_like(x)
            xs = jnp.concatenate([xh, x - xh, xh, zero], axis=0).astype(BF16)
            ys = jnp.concatenate([yh, yh, y - yh, zero], axis=0).astype(BF16)
            delta = lax.dot_general(xs, ys, (((0,), (0,)), ((), ())), preferred_element_type=F32)
            for i in range(far, count):
                w[i] = jnp.where(group, 0.0, w[i]) - delta[8 * i : 8 * i + 8]
        cols = ahead
        fill(g)
    return w


def aligned(x, m=16):
    return pl.multiple_of(x, m)


def stacked(hi, lo):
    return jnp.concatenate(
        [jnp.concatenate([hi, hi], axis=1), jnp.concatenate([lo, jnp.zeros_like(lo)], axis=1)], axis=0
    )


def fold(o):
    return o[:, :BS] + o[:, BS:]


def chol_kernel(pos_ref, plan_ref, mat_ref, out_ref, sol_ref, a_ref, hi_ref, lo_ref, inv_ref, winv_ref, wnext_ref, sem):
    n = G // BS
    copies = []
    for t, (i, j) in enumerate(TILES):
        copies.append(
            pltpu.make_async_copy(
                mat_ref.at[pl.ds(t * SB, SB)], a_ref.at[pl.ds(i * SB, SB), pl.ds(j * SB, SB)], sem.at[t]
            )
        )
        copies[-1].start()
    a_ref[pl.ds(G, EXTRA), :] = jnp.zeros((EXTRA, G), F32)
    for copy in copies:
        copy.wait()
    for j in range(NS):
        for h in range(2):
            a_ref[G : G + 1, j * SB + h * BS : j * SB + (h + 1) * BS] = a_ref[
                j * SB + h : j * SB + h + 1, j * SB + BS : (j + 1) * SB
            ]
    lane2 = lax.broadcasted_iota(jnp.int32, (BS, BS), 1)
    sub2 = lax.broadcasted_iota(jnp.int32, (BS, BS), 0)
    ext = pl.ds(G, EXTRA)

    def put(rows, cols, o):
        oh, ol = split(o)
        a_ref[rows, cols] = o
        hi_ref[rows, cols] = oh
        lo_ref[rows, cols] = ol
        return jnp.concatenate([oh, ol], axis=1)

    def solved(rows_list, cols):
        x = jnp.concatenate([a_ref[rows, cols] for rows in rows_list], axis=0)
        xh, xl = split(x)
        return fold(dot_nt(jnp.concatenate([xh, xl], axis=1), winv_ref[...]))

    def update(rows, erows, jc, pc):
        xh = jnp.concatenate([hi_ref[rows, pc], hi_ref[ext, pc]], axis=0)
        xl = jnp.concatenate([lo_ref[rows, pc], lo_ref[ext, pc]], axis=0)
        rh, rl = hi_ref[jc, pc], lo_ref[jc, pc]
        o = dot_nt(xh, rh) + dot_nt(xl, rh) + dot_nt(xh, rl)
        a_ref[rows, jc] = a_ref[rows, jc] - o[:SB]
        a_ref[erows, jc] = a_ref[erows, jc] - o[SB:]

    def step(k, carry):
        at = aligned(k * BS, BS)
        cols = pl.ds(at, BS)
        odd = lax.rem(k, 2)
        prev = pl.ds(aligned(jnp.maximum(k - 1, 0) * BS, BS), BS)
        edummy = DUMMY + SB
        eside = pl.ds(aligned(jnp.where(odd == 1, G, edummy)), EXTRA)

        def fill(g):
            if g < SIDES:
                base = plan_ref[k, g]
                rows = pl.ds(aligned(base), SB)
                o = solved([rows, eside] if g == 0 else [rows], prev)
                both = put(rows, prev, o[:SB])
                if g == 0:
                    both = jnp.concatenate([both, put(eside, prev, o[SB:])], axis=0)
                d = fold(dot_nt(both, wnext_ref[...]))
                drows = pl.ds(aligned(jnp.where(odd == 1, base, DUMMY)), SB)
                a_ref[drows, cols] = a_ref[drows, cols] - d[:SB]
                if g == 0:
                    a_ref[eside, cols] = a_ref[eside, cols] - d[SB:]
            elif g < SIDES + UNITS:
                u = SIDES + 4 * (g - SIDES)
                rows = pl.ds(aligned(plan_ref[k, u]), SB)
                jc = pl.ds(aligned(plan_ref[k, u + 1], SB), SB)
                pc = pl.ds(aligned(plan_ref[k, u + 2], SB), SB)
                update(rows, pl.ds(aligned(jnp.where(plan_ref[k, u + 3] == 1, G, edummy)), EXTRA), jc, pc)

        block = a_ref[pl.ds(at, BS), cols]
        w = eliminate([block[8 * i : 8 * i + 8] for i in range(BS // 8)], fill)
        w = jnp.concatenate(w, axis=0)
        inv = jnp.where(lane2 <= sub2, w, 0.0)
        inv_ref[pl.ds(at, BS), :] = inv
        ih, il = split(inv)
        winv_ref[...] = stacked(ih, il)

        @pl.when(odd == 0)
        def _():
            nxt = pl.ds(aligned(at + BS, BS), BS)
            o = solved([nxt], cols)
            both = put(nxt, cols, o)
            weights = stacked(both[:, :BS], both[:, BS:])
            wnext_ref[...] = weights
            a_ref[nxt, nxt] = a_ref[nxt, nxt] - fold(dot_nt(both, weights))

        @pl.when((odd == 1) & (k < n - 1))
        def _():
            nxt = pl.ds(aligned(at + BS, BS), SB)
            o = solved([nxt, ext], cols)
            put(nxt, cols, o[:SB])
            put(ext, cols, o[SB:])
            update(nxt, ext, nxt, pl.ds(aligned(at - BS, SB), SB))

        @pl.when(k == n - 1)
        def _():
            put(ext, cols, solved([ext], cols))

        put(pl.ds(at, BS), cols, jnp.where(lane2 == sub2, 1.0 / w, jnp.where(lane2 > sub2, w, 0.0)).T)
        return carry

    lax.fori_loop(0, n, step, 0)

    def back(s, c):
        k = n - 1 - s
        at = aligned(k * BS, BS)
        cols = pl.ds(at, BS)
        ih, il = split(inv_ref[pl.ds(at, BS), :])
        yh, yl = split(a_ref[pl.ds(G, 8), cols])
        y = jnp.concatenate([yh, yl], axis=0)
        z = dot_nn(y, ih)
        z = z[:8] + z[8:] + dot_nn(yh, il)
        sol_ref[:, cols] = z
        zh, zl = split(z)
        zz = jnp.concatenate([zh, zl], axis=0)
        wide = 4 * BS

        def sub(j, c2):
            jc = pl.ds(aligned(j * wide, wide), wide)
            o = dot_nn(zz, hi_ref[pl.ds(at, BS), jc])
            a_ref[pl.ds(G, 8), jc] = a_ref[pl.ds(G, 8), jc] - (o[:8] + o[8:] + dot_nn(zh, lo_ref[pl.ds(at, BS), jc]))
            return c2

        lax.fori_loop(0, (k + 3) // 4, sub, 0)
        return c

    lax.fori_loop(0, n, back, 0)

    p, q = pos_ref[0], pos_ref[1]
    for r in range(2):
        for c in range(2):
            rb = r * 8 + p
            cb = c * 8 + q
            blk = a_ref[pl.ds(aligned(rb * BS, BS), BS), pl.ds(aligned(cb * BS, BS), BS)]
            out_ref[r, :, c * BS : (c + 1) * BS] = jnp.where(rb >= cb, blk, 0.0)


def cholesky_call(pos, payload):
    return pl.pallas_call(
        chol_kernel,
        out_shape=(jax.ShapeDtypeStruct((2, BS, 2 * BS), F32), jax.ShapeDtypeStruct((8, G), F32)),
        in_specs=[
            pl.BlockSpec(memory_space=pltpu.SMEM),
            pl.BlockSpec(memory_space=pltpu.SMEM),
            pl.BlockSpec(memory_space=pl.ANY),
        ],
        out_specs=(pl.BlockSpec(memory_space=pltpu.VMEM), pl.BlockSpec(memory_space=pltpu.VMEM)),
        scratch_shapes=[
            pltpu.VMEM((TALL, G), F32),
            pltpu.VMEM((TALL, G), BF16),
            pltpu.VMEM((TALL, G), BF16),
            pltpu.VMEM((G, BS), F32),
            pltpu.VMEM((SB, SB), BF16),
            pltpu.VMEM((SB, SB), BF16),
            pltpu.SemaphoreType.DMA((len(TILES),)),
        ],
        compiler_params=pltpu.CompilerParams(vmem_limit_bytes=60 * 1024 * 1024),
        name="chol",
    )(pos, jnp.asarray(plan(), jnp.int32), payload)


def on_device(total, blocks, coefficients, residuals):
    payload = reduce_call(blocks, coefficients, residuals, 1.0 / total)
    pos = jnp.stack([lax.axis_index("gx"), lax.axis_index("gy")]).astype(jnp.int32)
    factor, answer = cholesky_call(pos, payload)
    return factor.reshape(1, 2, BS, 1, 2, BS), answer[0].reshape(G // BS, BS)


def solution(mesh):
    def whole(blocks, coefficients, residuals):
        spread = P(("gx", "gy", "gz"))
        return jax.shard_map(
            functools.partial(on_device, blocks.shape[0]),
            mesh=mesh,
            in_specs=(spread, spread, spread),
            out_specs=(P("gx", None, None, "gy", None, None), P()),
            check_vma=False,
        )(blocks, coefficients, residuals)

    return whole
```

```python
import functools

import jax
import jax.numpy as jnp
from jax import lax
from jax.experimental import pallas as pl
from jax.experimental.pallas import tpu as pltpu
from jax.sharding import PartitionSpec as P

G = 2048
BS = 128
SB = 2 * BS
NS = G // SB
EXTRA = 16
F32 = jnp.float32
BF16 = jnp.bfloat16
MESH = pl.DeviceIdType.MESH
ROUNDS = 3
SKEW = 1
STAGES = 10
STREAMS = 3 * ROUNDS
DIAG = [(j, j) for j in range(NS)]
SIDE = [(i, j) for j in range(NS) for i in range(j + 1, NS)]
TILES = DIAG[0::2] + SIDE[0::2] + DIAG[1::2] + SIDE[1::2]
ROWS = len(TILES) * SB
HALF = ROWS // 2
PART = HALF // STREAMS
UNITS_OF = (PART // 4, PART // 16, PART // 64)
ORDERS = ("xyz", "yzx", "zxy")


def split(x):
    hi = x.astype(BF16)
    return hi, (x - hi.astype(F32)).astype(BF16)


def dot_nt(a, b):
    return lax.dot_general(a, b, (((1,), (1,)), ((), ())), preferred_element_type=F32)


def dot_nn(a, b):
    return lax.dot_general(a, b, (((1,), (0,)), ((), ())), preferred_element_type=F32)


def lane_all(x, lane):
    return jnp.broadcast_to(x[:, lane : lane + 1], x.shape)


def row_all(x, row):
    return jnp.broadcast_to(x[row : row + 1, :], x.shape)


def place_of(x, y, z, core):
    return (lax.rem(y, 2) * 4 + x, z * 2 + core, y // 2)


def reduce_kernel(scale, blk_ref, coef_ref, res_ref, pay, design, flipped, outbox, inbox, work, near, far, swap_sem, rs_sem, ag_sem, end_sem):
    gx, gy, gz = lax.axis_index("gx"), lax.axis_index("gy"), lax.axis_index("gz")
    at = {"x": lax.rem(gx, 4), "y": gz * 2 + gx // 4, "z": gy // 2}
    core = lax.rem(gy, 2)

    def device(axis, shift):
        c = dict(at)
        c[axis] = lax.rem(c[axis] + shift + 4, 4)
        return place_of(c["x"], c["y"], c["z"], core)

    twin = place_of(at["x"], at["y"], at["z"], 1 - core)
    barrier = pltpu.get_barrier_semaphore()
    for axis in "xyz":
        for shift in (1, 2, 3):
            pl.semaphore_signal(barrier, inc=1, device_id=device(axis, shift), device_id_type=MESH)
    pl.semaphore_signal(barrier, inc=1, device_id=twin, device_id_type=MESH)

    obs = blk_ref.shape[0]
    slots = blk_ref.shape[1]
    step = 256

    def place(t, c):
        rows = pl.ds(pl.multiple_of(t * step, step), step)
        ids = [jnp.broadcast_to(blk_ref[rows, s : s + 1], (step, BS)) for s in range(slots)]
        vals = [coef_ref[rows, s * BS : (s + 1) * BS].astype(F32) for s in range(slots)]
        for b in range(G // BS):
            d = jnp.zeros((step, BS), F32)
            for s in range(slots):
                d = jnp.where(ids[s] == b, vals[s], d)
            db = d.astype(BF16)
            design[rows, b * BS : (b + 1) * BS] = db
            flipped[b * BS : (b + 1) * BS, rows] = db.T
        return c

    lax.fori_loop(0, obs // step, place, 0)

    res = res_ref[...]
    r1 = res.astype(BF16).astype(F32)
    r2 = (res - r1).astype(BF16).astype(F32)
    r3 = res - r1 - r2
    first = lax.broadcasted_iota(jnp.int32, (8, obs), 0)
    lhs = jnp.where(first == 0, r1, jnp.where(first == 1, r2, jnp.where(first == 2, r3, 0.0))).astype(BF16)

    def ds(start, size):
        return pl.ds(pl.multiple_of(start, 8), size)

    mine = core * HALF

    def gram(side, slot, dst, plus=None):
        (i0, j0), (i1, j1) = TILES[slot], TILES[slot + len(TILES) // 2]
        i = (i0 + (i1 - i0) * side) * SB
        j = (j0 + (j1 - j0) * side) * SB
        cols = design[:, pl.ds(pl.multiple_of(j, SB), SB)]
        base = slot * SB
        tile = dot_nn(flipped[pl.ds(pl.multiple_of(i, SB), SB), :], cols) * scale
        dst[base : base + SB, :] = tile if plus is None else tile + plus[base : base + SB, :]
        if i0 == j0:
            row = jnp.sum(dot_nn(lhs, cols), axis=0, keepdims=True) * scale
            rows = jnp.concatenate([row[:, :BS], row[:, BS:], jnp.zeros((6, BS), F32)], axis=0)
            dst[base : base + 8, BS:] = rows if plus is None else rows + plus[base : base + 8, BS:]

    started = []

    def remote(src, dst, sems, to):
        copy = pltpu.make_async_remote_copy(
            src_ref=src, dst_ref=dst, send_sem=sems.at[0], recv_sem=sems.at[1], device_id=to, device_id_type=MESH
        )
        copy.start()
        started.append(copy)
        return copy

    def add(dst, dst_start, srcs, src_start, size, goal=None):
        piece = min(size, 64)
        goal, goal_start = (dst, dst_start) if goal is None else goal

        def body(t, carry):
            total = dst[ds(dst_start + t * piece, piece), :]
            for src in srcs:
                total = total + src[ds(src_start + t * piece, piece), :]
            goal[ds(goal_start + t * piece, piece), :] = total
            return carry

        if size == piece:
            body(0, 0)
        else:
            lax.fori_loop(0, size // piece, body, 0)

    class Stream:
        def __init__(self, s):
            self.s = s
            self.order = ORDERS[s % 3]
            self.base = s * PART
            self.pieces = []

        def swap(self):
            rows = PART * self.s
            self.swapped = remote(outbox.at[ds(rows, PART)], inbox.at[ds(rows, PART)], swap_sem.at[self.s], twin)

        def opposite(self):
            s, unit = self.s, UNITS_OF[0]
            piece, axis = self.enter(0), self.order[0]
            half = unit // 2
            self.a = remote(work.at[ds(piece(2), half)], near.at[s, ds(0, half)], rs_sem.at[s, 0, 0], device(axis, 1))
            self.b = remote(
                work.at[ds(piece(2) + half, half)], near.at[s, ds(half, half)], rs_sem.at[s, 0, 1], device(axis, -1)
            )

        def enter(self, p):
            m, base, unit = at[self.order[p]], self.base, UNITS_OF[p]
            self.pieces.append(lambda i: base + lax.rem(m + i + 4, 4) * unit)
            return self.pieces[p]

        def sides(self):
            s, unit, axis, piece = self.s, UNITS_OF[0], self.order[0], self.pieces[0]
            half = unit // 2
            self.a.wait_recv()
            add(work, piece(1), (near.at[s],), 0, half)
            u = remote(work.at[ds(piece(1), unit)], far.at[s, 0, ds(0, unit)], rs_sem.at[s, 0, 2], device(axis, 1))
            self.b.wait_recv()
            add(work, piece(-1) + half, (near.at[s],), half, half)
            d = remote(work.at[ds(piece(-1), unit)], far.at[s, 1, ds(0, unit)], rs_sem.at[s, 0, 3], device(axis, -1))
            self.wait = (u, d)

        def finish(self, p):
            for copy in self.wait:
                copy.wait_recv()
            self.base = self.pieces[p](0)
            goal = (pay, mine + self.base) if p == 2 else None
            srcs = tuple(far.at[self.s, k] for k in range(len(self.wait)))
            add(work, self.base, srcs, sum(UNITS_OF[:p]), UNITS_OF[p], goal)

        def exchange(self, p):
            self.finish(p - 1)
            s, unit, piece, axis = self.s, UNITS_OF[p], self.enter(p), self.order[p]
            off = sum(UNITS_OF[:p])
            self.wait = tuple(
                remote(work.at[ds(piece(i), unit)], far.at[s, i - 1, ds(off, unit)], rs_sem.at[s, p, i - 1], device(axis, i))
                for i in (1, 2, 3)
            )

        def spread(self, p):
            s, unit, axis, piece = self.s, UNITS_OF[p], self.order[p], self.pieces[p]
            if p == 2:
                self.finish(2)
            else:
                for copy in self.wait:
                    copy.wait_recv()
            own = pay.at[ds(mine + piece(0), unit)]
            shifts = (1, 2, 3) if p else (1, 3)
            self.wait = tuple(remote(own, own, ag_sem.at[s, p, i - 1], device(axis, i)) for i in shifts)
            if p == 0:
                self.ends = [remote(own, own, end_sem.at[s, 0], twin)]

        def relay(self):
            s, unit, axis, piece = self.s, UNITS_OF[0], self.order[0], self.pieces[0]
            half = unit // 2
            u, d = self.wait
            u.wait_recv()
            part = pay.at[ds(mine + piece(-1), half)]
            up = remote(part, part, ag_sem.at[s, 0, 1], device(axis, 1))
            d.wait_recv()
            part = pay.at[ds(mine + piece(1) + half, half)]
            down = remote(part, part, ag_sem.at[s, 0, 3], device(axis, -1))
            self.wait = (up, down)
            for k, i in ((1, -1), (2, 1)):
                part = pay.at[ds(mine + piece(i), unit)]
                self.ends.append(remote(part, part, end_sem.at[s, k], twin))

        def tail(self):
            for copy in self.wait:
                copy.wait_recv()
            part = pay.at[ds(mine + self.pieces[0](2), UNITS_OF[0])]
            self.ends.append(remote(part, part, end_sem.at[self.s, 3], twin))

        def end(self):
            for copy in self.ends:
                copy.wait_recv()

        def run(self, stage):
            if stage == 0:
                self.opposite()
            elif stage == 1:
                self.sides()
            elif stage < 4:
                self.exchange(stage - 1)
            elif stage < 7:
                self.spread(6 - stage)
            elif stage == 7:
                self.relay()
            elif stage == 8:
                self.tail()
            else:
                self.end()

    streams = [Stream(s) for s in range(STREAMS)]
    per = PART // SB

    def give(r):
        for s in range(3 * r, 3 * r + 3):
            for k in range(per):
                gram(1 - core, s * per + k, outbox)
            if s == 0:
                pl.semaphore_wait(barrier, 10)
            streams[s].swap()

    def keep(r):
        for s in range(3 * r, 3 * r + 3):
            streams[s].swapped.wait_recv()
            for k in range(per):
                gram(core, s * per + k, work, inbox)
            streams[s].run(0)

    give(0)
    for t in range(STAGES + SKEW * (ROUNDS - 1)):
        for r in reversed(range(ROUNDS)):
            stage = t - SKEW * r
            if stage == 0:
                if r + 1 < ROUNDS:
                    give(r + 1)
                keep(r)
            elif 0 < stage < STAGES:
                for c in range(3):
                    streams[3 * r + c].run(stage)
    for copy in started:
        copy.wait_send()


def reduce_call(blocks, coefficients, residuals, scale):
    obs = blocks.shape[0]
    units = sum(UNITS_OF)
    return pl.pallas_call(
        functools.partial(reduce_kernel, scale),
        out_shape=jax.ShapeDtypeStruct((ROWS, SB), F32),
        in_specs=[pl.BlockSpec(memory_space=pltpu.VMEM)] * 3,
        out_specs=pl.BlockSpec(memory_space=pltpu.VMEM),
        scratch_shapes=[
            pltpu.VMEM((obs, G), BF16),
            pltpu.VMEM((G, obs), BF16),
            pltpu.VMEM((HALF, SB), F32),
            pltpu.VMEM((HALF, SB), F32),
            pltpu.VMEM((HALF, SB), F32),
            pltpu.VMEM((STREAMS, UNITS_OF[0], SB), F32),
            pltpu.VMEM((STREAMS, 3, units, SB), F32),
            pltpu.SemaphoreType.DMA((STREAMS, 2)),
            pltpu.SemaphoreType.DMA((STREAMS, 3, 4, 2)),
            pltpu.SemaphoreType.DMA((STREAMS, 3, 4, 2)),
            pltpu.SemaphoreType.DMA((STREAMS, 4, 2)),
        ],
        compiler_params=pltpu.CompilerParams(
            vmem_limit_bytes=60 * 1024 * 1024, collective_id=0, has_side_effects=True
        ),
        name="reduce",
    )(blocks, coefficients.reshape(obs, -1), residuals.reshape(1, obs))


SPLITS = (6, 12, 16)
DUMMY = G + EXTRA
TALL = DUMMY + SB + EXTRA
UNITS = 7
SOLVES = 2
LAG = 2
FIRST_UNIT = 6
SIDES = NS - 1


def plan():
    n = 2 * NS
    sides = [[DUMMY] * SIDES for _ in range(n)]
    units = [[(DUMMY, 0, 0, 0)] * UNITS for _ in range(n)]
    todo = []
    for k in range(n):
        if k:
            first = (k - 1) // 2 + (1 if k % 2 else 2)
            for t, i in enumerate(range(first, NS)):
                sides[k][t] = i * SB
        if k >= 2 and k % 2 == 0:
            p = k // 2 - 1
            for j in range(p + 1, NS):
                for i in range(j, NS):
                    if (i, j) != (p + 1, p + 1):
                        todo.append((2 * j if i > j else 2 * j - 1, j, p, i))
        todo.sort()
        now, todo = todo[:UNITS], todo[UNITS:]
        for t, (limit, j, p, i) in enumerate(now):
            assert limit >= k
            units[k][t] = (i * SB, j * SB, p * SB, 1 if i == j else 0)
    assert not todo
    flat = []
    for k in range(n):
        flat.append(sides[k] + [v for u in units[k] for v in u])
    return flat


def eliminate(w, fill):
    lane = lax.broadcasted_iota(jnp.int32, (8, BS), 1)
    sub = lax.broadcasted_iota(jnp.int32, (8, BS), 0)
    w = list(w)
    count = len(w)
    start = 0
    for g in range(count):
        end = min(e for e in SPLITS if e > g)
        if g == start:
            cols = [lane_all(w[g], 8 * g + j) for j in range(8)]
        r = w[g]
        group = (lane >= 8 * g) & (lane < 8 * g + 8)
        near = range(g + 1, end)
        raw = {i: [lane_all(w[i], 8 * g + j) for j in range(8)] for i in near}
        ahead = [lane_all(w[g + 1], 8 * g + 8 + j) for j in range(8)] if g + 1 < end else None
        accs = {i: jnp.where(group, 0.0, w[i]) for i in near}
        pivot = row_all(cols[0], 0)
        for j in range(8):
            root = lax.rsqrt(pivot)
            if j < 7:
                pivot = row_all(cols[j + 1], j + 1) - (row_all(cols[j], j + 1) * root) * (row_all(cols[j + 1], j) * root)
            scaled = cols[j] * root
            below = jnp.where(sub > j, scaled, 0.0)
            here = lane == 8 * g + j
            row = row_all(jnp.where(here, 1.0, r), j) * root
            r = jnp.where(sub == j, row, jnp.where(here & (sub > j), 0.0, r) - below * row)
            ups = {}
            for l in range(j + 1, 8):
                ups[l] = row_all(cols[l], j) * root
                cols[l] = cols[l] - scaled * ups[l]
            inverse_row = jnp.where((lane > 8 * g + j) & (lane < 8 * g + 8), 0.0, row)
            for i in near:
                c = raw[i]
                m = c[j] * root
                for l in range(j + 1, 8):
                    c[l] = c[l] - m * ups[l]
                accs[i] = accs[i] - m * inverse_row
                if i == g + 1:
                    ahead = [ahead[l] - m * row_all(m, l) for l in range(8)]
        w[g] = r
        for i in near:
            w[i] = accs[i]
        if g + 1 == end and end < count:
            xs, ys = [], []
            for i in range(start, end):
                xs.append(jnp.where(lane >= 8 * end, w[i], 0.0))
                ys.append(jnp.where((lane < 8 * end) & (lane > 8 * i + sub), 0.0, w[i]))
            xh, xl = split(jnp.concatenate(xs, axis=0))
            yh, yl = split(jnp.concatenate(ys, axis=0))
            delta = lax.dot_general(
                jnp.concatenate([xh, xl, xh], axis=0),
                jnp.concatenate([yh, yh, yl], axis=0),
                (((0,), (0,)), ((), ())),
                preferred_element_type=F32,
            )
            done = (lane >= 8 * start) & (lane < 8 * end)
            for i in range(end, count):
                w[i] = jnp.where(done, 0.0, w[i]) - delta[8 * i : 8 * i + 8]
            start = end
        cols = ahead
        fill(g)
    return w


def aligned(x, m=16):
    return pl.multiple_of(x, m)


def stacked(hi, lo):
    return jnp.concatenate(
        [jnp.concatenate([hi, hi], axis=1), jnp.concatenate([lo, jnp.zeros_like(lo)], axis=1)], axis=0
    )


def fold(o):
    return o[:, :BS] + o[:, BS:]


def chol_kernel(plan_ref, mat_ref, out_ref, sol_ref, a_ref, hi_ref, lo_ref, inv_ref, winv_ref, wnext_ref, y_ref, sem):
    n = G // BS
    copies = []
    for t, (i, j) in enumerate(TILES):
        copies.append(
            pltpu.make_async_copy(
                mat_ref.at[pl.ds(t * SB, SB)], a_ref.at[pl.ds(i * SB, SB), pl.ds(j * SB, SB)], sem.at[t]
            )
        )
        copies[-1].start()
    a_ref[pl.ds(G, EXTRA), :] = jnp.zeros((EXTRA, G), F32)
    for copy in copies:
        copy.wait()
    for j in range(NS):
        for h in range(2):
            a_ref[G : G + 1, j * SB + h * BS : j * SB + (h + 1) * BS] = a_ref[
                j * SB + h : j * SB + h + 1, j * SB + BS : (j + 1) * SB
            ]
    lane2 = lax.broadcasted_iota(jnp.int32, (BS, BS), 1)
    sub2 = lax.broadcasted_iota(jnp.int32, (BS, BS), 0)
    ext = pl.ds(G, EXTRA)

    def put(rows, cols, o):
        oh, ol = split(o)
        hi_ref[rows, cols] = oh
        lo_ref[rows, cols] = ol
        return jnp.concatenate([oh, ol], axis=1)

    def solved(rows_list, cols):
        x = jnp.concatenate([a_ref[rows, cols] for rows in rows_list], axis=0)
        xh, xl = split(x)
        return fold(dot_nt(jnp.concatenate([xh, xl], axis=1), winv_ref[...]))

    def update(rows, erows, jc, pc):
        xh = jnp.concatenate([hi_ref[rows, pc], hi_ref[ext, pc]], axis=0)
        xl = jnp.concatenate([lo_ref[rows, pc], lo_ref[ext, pc]], axis=0)
        rh, rl = hi_ref[jc, pc], lo_ref[jc, pc]
        o = dot_nt(xh, rh) + dot_nt(xl, rh) + dot_nt(xh, rl)
        a_ref[rows, jc] = a_ref[rows, jc] - o[:SB]
        a_ref[erows, jc] = a_ref[erows, jc] - o[SB:]

    def step(k, carry):
        at = aligned(k * BS, BS)
        cols = pl.ds(at, BS)
        odd = lax.rem(k, 2)
        prev = pl.ds(aligned(jnp.maximum(k - 1, 0) * BS, BS), BS)
        edummy = DUMMY + SB
        eside = pl.ds(aligned(jnp.where(odd == 1, G, edummy)), EXTRA)

        waiting = {}

        def solve_side(t):
            rows = pl.ds(aligned(plan_ref[k, t]), SB)
            o = solved([rows, eside] if t == 0 else [rows], prev)
            both = put(rows, prev, o[:SB])
            if t == 0:
                both = jnp.concatenate([both, put(eside, prev, o[SB:])], axis=0)
            waiting[t] = both

        def update_side(t):
            d = fold(dot_nt(waiting.pop(t), wnext_ref[...]))
            rows = pl.ds(aligned(jnp.where(odd == 1, plan_ref[k, t], DUMMY)), SB)
            a_ref[rows, cols] = a_ref[rows, cols] - d[:SB]
            if t == 0:
                a_ref[eside, cols] = a_ref[eside, cols] - d[SB:]

        def tile_update(t):
            u = SIDES + 4 * t
            rows = pl.ds(aligned(plan_ref[k, u]), SB)
            jc = pl.ds(aligned(plan_ref[k, u + 1], SB), SB)
            pc = pl.ds(aligned(plan_ref[k, u + 2], SB), SB)
            update(rows, pl.ds(aligned(jnp.where(plan_ref[k, u + 3] == 1, G, edummy)), EXTRA), jc, pc)

        def fill(g):
            for t in range(SIDES):
                if t // SOLVES == g:
                    solve_side(t)
            for t in range(SIDES):
                if t // SOLVES + LAG == g:
                    update_side(t)
            if FIRST_UNIT <= g < FIRST_UNIT + UNITS:
                tile_update(g - FIRST_UNIT)

        block = a_ref[pl.ds(at, BS), cols]
        w = eliminate([block[8 * i : 8 * i + 8] for i in range(BS // 8)], fill)
        w = jnp.concatenate(w, axis=0)
        inv = jnp.where(lane2 <= sub2, w, 0.0)
        inv_ref[pl.ds(at, BS), :] = inv
        ih, il = split(inv)
        winv_ref[...] = stacked(ih, il)

        @pl.when(odd == 0)
        def _():
            nxt = pl.ds(aligned(at + BS, BS), BS)
            o = solved([nxt], cols)
            both = put(nxt, cols, o)
            weights = stacked(both[:, :BS], both[:, BS:])
            wnext_ref[...] = weights
            a_ref[nxt, nxt] = a_ref[nxt, nxt] - fold(dot_nt(both, weights))

        @pl.when((odd == 1) & (k < n - 1))
        def _():
            nxt = pl.ds(aligned(at + BS, BS), SB)
            o = solved([nxt, ext], cols)
            put(nxt, cols, o[:SB])
            put(ext, cols, o[SB:])
            update(nxt, ext, nxt, pl.ds(aligned(at - BS, SB), SB))

        @pl.when(k == n - 1)
        def _():
            put(ext, cols, solved([ext], cols))

        a_ref[pl.ds(at, BS), cols] = jnp.where(lane2 == sub2, 1.0 / w, jnp.where(lane2 > sub2, w, 0.0)).T
        return carry

    lax.fori_loop(0, n, step, 0)

    def back(s, c):
        k = n - 1 - s
        at = aligned(k * BS, BS)
        cols = pl.ds(at, BS)
        ih, il = split(inv_ref[pl.ds(at, BS), :])
        yh, yl = split(y_ref[:, cols])
        y = jnp.concatenate([yh, yl], axis=0)
        z = dot_nn(y, ih)
        z = z[:8] + z[8:] + dot_nn(yh, il)
        sol_ref[pl.ds(k, 1), :] = z[:1]
        zh, zl = split(z)
        zz = jnp.concatenate([zh, zl], axis=0)
        wide = 4 * BS

        def sub(j, c2):
            jc = pl.ds(aligned(j * wide, wide), wide)
            o = dot_nn(zz, hi_ref[pl.ds(at, BS), jc])
            y_ref[:, jc] = y_ref[:, jc] - (o[:8] + o[8:] + dot_nn(zh, lo_ref[pl.ds(at, BS), jc]))
            return c2

        lax.fori_loop(0, (k + 3) // 4, sub, 0)
        return c

    y_ref[...] = hi_ref[ext, :].astype(F32)[:8] + lo_ref[ext, :].astype(F32)[:8]
    lax.fori_loop(0, n, back, 0)

    p, q = lax.axis_index("gx"), lax.axis_index("gy")
    for r in range(2):
        for c in range(2):
            rb = r * 8 + p
            cb = c * 8 + q
            rows = pl.ds(aligned(rb * BS, BS), BS)
            cols = pl.ds(aligned(cb * BS, BS), BS)
            off = hi_ref[rows, cols].astype(F32) + lo_ref[rows, cols].astype(F32)
            out_ref[r, :, c, :] = jnp.where(rb > cb, off, jnp.where(rb == cb, a_ref[rows, cols], 0.0))


def cholesky_call(payload):
    return pl.pallas_call(
        chol_kernel,
        out_shape=(jax.ShapeDtypeStruct((2, BS, 2, BS), F32), jax.ShapeDtypeStruct((G // BS, BS), F32)),
        in_specs=[
            pl.BlockSpec(memory_space=pltpu.SMEM),
            pl.BlockSpec(memory_space=pl.ANY),
        ],
        out_specs=(pl.BlockSpec(memory_space=pltpu.VMEM), pl.BlockSpec(memory_space=pltpu.VMEM)),
        scratch_shapes=[
            pltpu.VMEM((TALL, G), F32),
            pltpu.VMEM((TALL, G), BF16),
            pltpu.VMEM((TALL, G), BF16),
            pltpu.VMEM((G, BS), F32),
            pltpu.VMEM((SB, SB), BF16),
            pltpu.VMEM((SB, SB), BF16),
            pltpu.VMEM((8, G), F32),
            pltpu.SemaphoreType.DMA((len(TILES),)),
        ],
        compiler_params=pltpu.CompilerParams(vmem_limit_bytes=60 * 1024 * 1024),
        name="chol",
    )(jnp.asarray(plan(), jnp.int32), payload)


def on_device(total, blocks, coefficients, residuals):
    payload = reduce_call(blocks, coefficients, residuals, 1.0 / total)
    factor, answer = cholesky_call(payload)
    return factor.reshape(1, 2, BS, 1, 2, BS), answer


def solution(mesh):
    def whole(blocks, coefficients, residuals):
        spread = P(("gx", "gy", "gz"))
        return jax.shard_map(
            functools.partial(on_device, blocks.shape[0]),
            mesh=mesh,
            in_specs=(spread, spread, spread),
            out_specs=(P("gx", None, None, "gy", None, None), P()),
            check_vma=False,
        )(blocks, coefficients, residuals)

    return whole
```

```python
import functools

import jax
import jax.numpy as jnp
from jax import lax
from jax.experimental import pallas as pl
from jax.experimental.pallas import tpu as pltpu
from jax.sharding import PartitionSpec as P

G = 2048
BS = 128
SB = 2 * BS
NS = G // SB
EXTRA = 16
F32 = jnp.float32
BF16 = jnp.bfloat16
MESH = pl.DeviceIdType.MESH
ROUNDS = 3
SKEW = 1
RED_MB = 34
CHOL_MB = 44
STAGES = 10
STREAMS = 3 * ROUNDS
DIAG = [(j, j) for j in range(NS)]
SIDE = [(i, j) for j in range(NS) for i in range(j + 1, NS)]
TILES = DIAG[0::2] + SIDE[0::2] + DIAG[1::2] + SIDE[1::2]
ROWS = len(TILES) * SB
HALF = ROWS // 2
PART = HALF // STREAMS
UNITS_OF = (PART // 4, PART // 16, PART // 64)
ORDERS = ("xyz", "yzx", "zxy")


def split(x):
    hi = x.astype(BF16)
    return hi, (x - hi.astype(F32)).astype(BF16)


def dot_nt(a, b):
    return lax.dot_general(a, b, (((1,), (1,)), ((), ())), preferred_element_type=F32)


def dot_nn(a, b):
    return lax.dot_general(a, b, (((1,), (0,)), ((), ())), preferred_element_type=F32)


def lane_all(x, lane):
    return jnp.broadcast_to(x[:, lane : lane + 1], x.shape)


def row_all(x, row):
    return jnp.broadcast_to(x[row : row + 1, :], x.shape)


def place_of(x, y, z, core):
    return (lax.rem(y, 2) * 4 + x, z * 2 + core, y // 2)


def reduce_kernel(scale, blk_ref, coef_ref, res_ref, pay, design, flipped, outbox, inbox, work, near, far, swap_sem, rs_sem, ag_sem, end_sem):
    gx, gy, gz = lax.axis_index("gx"), lax.axis_index("gy"), lax.axis_index("gz")
    at = {"x": lax.rem(gx, 4), "y": gz * 2 + gx // 4, "z": gy // 2}
    core = lax.rem(gy, 2)

    def device(axis, shift):
        c = dict(at)
        c[axis] = lax.rem(c[axis] + shift + 4, 4)
        return place_of(c["x"], c["y"], c["z"], core)

    twin = place_of(at["x"], at["y"], at["z"], 1 - core)
    barrier = pltpu.get_barrier_semaphore()
    for axis in "xyz":
        for shift in (1, 2, 3):
            pl.semaphore_signal(barrier, inc=1, device_id=device(axis, shift), device_id_type=MESH)
    pl.semaphore_signal(barrier, inc=1, device_id=twin, device_id_type=MESH)

    slots, obs = blk_ref.shape
    step = 256

    def place(t, c):
        rows = pl.ds(pl.multiple_of(t * step, step), step)
        ids = [jnp.broadcast_to(blk_ref[s : s + 1, rows], (BS, step)).T for s in range(slots)]
        vals = [coef_ref[rows, s * BS : (s + 1) * BS].astype(F32) for s in range(slots)]
        for b in range(G // BS):
            d = jnp.zeros((step, BS), F32)
            for s in range(slots):
                d = jnp.where(ids[s] == b, vals[s], d)
            db = d.astype(BF16)
            design[rows, b * BS : (b + 1) * BS] = db
            flipped[b * BS : (b + 1) * BS, rows] = db.T
        return c

    lax.fori_loop(0, obs // step, place, 0)

    res = res_ref[...]
    r1 = res.astype(BF16).astype(F32)
    r2 = (res - r1).astype(BF16).astype(F32)
    r3 = res - r1 - r2
    first = lax.broadcasted_iota(jnp.int32, (8, obs), 0)
    lhs = jnp.where(first == 0, r1, jnp.where(first == 1, r2, jnp.where(first == 2, r3, 0.0))).astype(BF16)

    def ds(start, size):
        return pl.ds(pl.multiple_of(start, 8), size)

    mine = core * HALF

    def gram(side, slot, dst, plus=None):
        (i0, j0), (i1, j1) = TILES[slot], TILES[slot + len(TILES) // 2]
        i = (i0 + (i1 - i0) * side) * SB
        j = (j0 + (j1 - j0) * side) * SB
        cols = design[:, pl.ds(pl.multiple_of(j, SB), SB)]
        base = slot * SB
        tile = dot_nn(flipped[pl.ds(pl.multiple_of(i, SB), SB), :], cols) * scale
        dst[base : base + SB, :] = tile if plus is None else tile + plus[base : base + SB, :]
        if i0 == j0:
            row = jnp.sum(dot_nn(lhs, cols), axis=0, keepdims=True) * scale
            rows = jnp.concatenate([row[:, :BS], row[:, BS:], jnp.zeros((6, BS), F32)], axis=0)
            dst[base : base + 8, BS:] = rows if plus is None else rows + plus[base : base + 8, BS:]

    started = []

    def remote(src, dst, sems, to):
        copy = pltpu.make_async_remote_copy(
            src_ref=src, dst_ref=dst, send_sem=sems.at[0], recv_sem=sems.at[1], device_id=to, device_id_type=MESH
        )
        copy.start()
        started.append(copy)
        return copy

    def add(dst, dst_start, srcs, src_start, size, goal=None):
        piece = min(size, 64)
        goal, goal_start = (dst, dst_start) if goal is None else goal

        def body(t, carry):
            total = dst[ds(dst_start + t * piece, piece), :]
            for src in srcs:
                total = total + src[ds(src_start + t * piece, piece), :]
            goal[ds(goal_start + t * piece, piece), :] = total
            return carry

        if size == piece:
            body(0, 0)
        else:
            lax.fori_loop(0, size // piece, body, 0)

    class Stream:
        def __init__(self, s):
            self.s = s
            self.order = ORDERS[s % 3]
            self.base = s * PART
            self.pieces = []

        def swap(self):
            rows = PART * self.s
            self.swapped = remote(outbox.at[ds(rows, PART)], inbox.at[ds(rows, PART)], swap_sem.at[self.s], twin)

        def opposite(self):
            s, unit = self.s, UNITS_OF[0]
            piece, axis = self.enter(0), self.order[0]
            half = unit // 2
            self.a = remote(work.at[ds(piece(2), half)], near.at[s, ds(0, half)], rs_sem.at[s, 0, 0], device(axis, 1))
            self.b = remote(
                work.at[ds(piece(2) + half, half)], near.at[s, ds(half, half)], rs_sem.at[s, 0, 1], device(axis, -1)
            )

        def enter(self, p):
            m, base, unit = at[self.order[p]], self.base, UNITS_OF[p]
            self.pieces.append(lambda i: base + lax.rem(m + i + 4, 4) * unit)
            return self.pieces[p]

        def sides(self):
            s, unit, axis, piece = self.s, UNITS_OF[0], self.order[0], self.pieces[0]
            half = unit // 2
            self.a.wait_recv()
            add(work, piece(1), (near.at[s],), 0, half)
            u = remote(work.at[ds(piece(1), unit)], far.at[s, 0, ds(0, unit)], rs_sem.at[s, 0, 2], device(axis, 1))
            self.b.wait_recv()
            add(work, piece(-1) + half, (near.at[s],), half, half)
            d = remote(work.at[ds(piece(-1), unit)], far.at[s, 1, ds(0, unit)], rs_sem.at[s, 0, 3], device(axis, -1))
            self.wait = (u, d)

        def finish(self, p):
            for copy in self.wait:
                copy.wait_recv()
            self.base = self.pieces[p](0)
            goal = (pay, mine + self.base) if p == 2 else None
            srcs = tuple(far.at[self.s, k] for k in range(len(self.wait)))
            add(work, self.base, srcs, sum(UNITS_OF[:p]), UNITS_OF[p], goal)

        def exchange(self, p):
            self.finish(p - 1)
            s, unit, piece, axis = self.s, UNITS_OF[p], self.enter(p), self.order[p]
            off = sum(UNITS_OF[:p])
            self.wait = tuple(
                remote(work.at[ds(piece(i), unit)], far.at[s, i - 1, ds(off, unit)], rs_sem.at[s, p, i - 1], device(axis, i))
                for i in (1, 2, 3)
            )

        def spread(self, p):
            s, unit, axis, piece = self.s, UNITS_OF[p], self.order[p], self.pieces[p]
            if p == 2:
                self.finish(2)
            else:
                for copy in self.wait:
                    copy.wait_recv()
            own = pay.at[ds(mine + piece(0), unit)]
            shifts = (1, 2, 3) if p else (1, 3)
            self.wait = tuple(remote(own, own, ag_sem.at[s, p, i - 1], device(axis, i)) for i in shifts)
            if p == 0:
                self.ends = [remote(own, own, end_sem.at[s, 0], twin)]

        def relay(self):
            s, unit, axis, piece = self.s, UNITS_OF[0], self.order[0], self.pieces[0]
            half = unit // 2
            u, d = self.wait
            u.wait_recv()
            part = pay.at[ds(mine + piece(-1), half)]
            up = remote(part, part, ag_sem.at[s, 0, 1], device(axis, 1))
            d.wait_recv()
            part = pay.at[ds(mine + piece(1) + half, half)]
            down = remote(part, part, ag_sem.at[s, 0, 3], device(axis, -1))
            self.wait = (up, down)
            for k, i in ((1, -1), (2, 1)):
                part = pay.at[ds(mine + piece(i), unit)]
                self.ends.append(remote(part, part, end_sem.at[s, k], twin))

        def tail(self):
            for copy in self.wait:
                copy.wait_recv()
            part = pay.at[ds(mine + self.pieces[0](2), UNITS_OF[0])]
            self.ends.append(remote(part, part, end_sem.at[self.s, 3], twin))

        def end(self):
            for copy in self.ends:
                copy.wait_recv()

        def run(self, stage):
            if stage == 0:
                self.opposite()
            elif stage == 1:
                self.sides()
            elif stage < 4:
                self.exchange(stage - 1)
            elif stage < 7:
                self.spread(6 - stage)
            elif stage == 7:
                self.relay()
            elif stage == 8:
                self.tail()
            else:
                self.end()

    streams = [Stream(s) for s in range(STREAMS)]
    per = PART // SB

    def give(r):
        for s in range(3 * r, 3 * r + 3):
            for k in range(per):
                gram(1 - core, s * per + k, outbox)
            if s == 0:
                pl.semaphore_wait(barrier, 10)
            streams[s].swap()

    def keep(r):
        for s in range(3 * r, 3 * r + 3):
            streams[s].swapped.wait_recv()
            for k in range(per):
                gram(core, s * per + k, work, inbox)
            streams[s].run(0)

    give(0)
    for t in range(STAGES + SKEW * (ROUNDS - 1)):
        for r in reversed(range(ROUNDS)):
            stage = t - SKEW * r
            if stage == 0:
                if r + 1 < ROUNDS:
                    give(r + 1)
                keep(r)
            elif 0 < stage < STAGES:
                for c in range(3):
                    streams[3 * r + c].run(stage)
    for copy in started:
        copy.wait_send()


def reduce_call(blocks, coefficients, residuals, scale):
    obs = blocks.shape[0]
    units = sum(UNITS_OF)
    return pl.pallas_call(
        functools.partial(reduce_kernel, scale),
        out_shape=jax.ShapeDtypeStruct((ROWS, SB), F32),
        in_specs=[pl.BlockSpec(memory_space=pltpu.VMEM)] * 3,
        out_specs=pl.BlockSpec(memory_space=pltpu.VMEM),
        scratch_shapes=[
            pltpu.VMEM((obs, G), BF16),
            pltpu.VMEM((G, obs), BF16),
            pltpu.VMEM((HALF, SB), F32),
            pltpu.VMEM((HALF, SB), F32),
            pltpu.VMEM((HALF, SB), F32),
            pltpu.VMEM((STREAMS, UNITS_OF[0], SB), F32),
            pltpu.VMEM((STREAMS, 3, units, SB), F32),
            pltpu.SemaphoreType.DMA((STREAMS, 2)),
            pltpu.SemaphoreType.DMA((STREAMS, 3, 4, 2)),
            pltpu.SemaphoreType.DMA((STREAMS, 3, 4, 2)),
            pltpu.SemaphoreType.DMA((STREAMS, 4, 2)),
        ],
        compiler_params=pltpu.CompilerParams(
            vmem_limit_bytes=RED_MB * 1024 * 1024, collective_id=0, has_side_effects=True
        ),
        name="reduce",
    )(blocks.T, coefficients.reshape(obs, -1), residuals.reshape(1, obs))


SPLITS = (6, 12, 16)
DUMMY = G + EXTRA
TALL = DUMMY + SB + EXTRA
SEGMENTS = ((0, 8, 7, 7), (8, 14, 3, 6), (14, 16, 1, 0))
UNITS = 7
SOLVES = 2
LAG = 2
FIRST_UNIT = 6
SIDES = NS - 1


def plan():
    n = 2 * NS
    sides = [[DUMMY] * SIDES for _ in range(n)]
    units = [[(DUMMY, 0, 0, 0)] * UNITS for _ in range(n)]
    todo = []
    for k in range(n):
        if k:
            first = (k - 1) // 2 + (1 if k % 2 else 2)
            for t, i in enumerate(range(first, NS)):
                sides[k][t] = i * SB
        if k >= 2 and k % 2 == 0:
            p = k // 2 - 1
            for j in range(p + 1, NS):
                for i in range(j, NS):
                    if (i, j) != (p + 1, p + 1):
                        todo.append((2 * j if i > j else 2 * j - 1, j, p, i))
        todo.sort()
        room = next(u for a, b, _, u in SEGMENTS if a <= k < b)
        now, todo = todo[:room], todo[room:]
        for t, (limit, j, p, i) in enumerate(now):
            assert limit >= k
            units[k][t] = (i * SB, j * SB, p * SB, 1 if i == j else 0)
    assert not todo
    flat = []
    for k in range(n):
        flat.append(sides[k] + [v for u in units[k] for v in u])
    return flat


def eliminate(w, fill):
    lane = lax.broadcasted_iota(jnp.int32, (8, BS), 1)
    sub = lax.broadcasted_iota(jnp.int32, (8, BS), 0)
    w = list(w)
    count = len(w)
    start = 0
    for g in range(count):
        end = min(e for e in SPLITS if e > g)
        if g == start:
            cols = [lane_all(w[g], 8 * g + j) for j in range(8)]
        r = w[g]
        group = (lane >= 8 * g) & (lane < 8 * g + 8)
        near = range(g + 1, end)
        raw = {i: [lane_all(w[i], 8 * g + j) for j in range(8)] for i in near}
        ahead = [lane_all(w[g + 1], 8 * g + 8 + j) for j in range(8)] if g + 1 < end else None
        accs = {i: jnp.where(group, 0.0, w[i]) for i in near}
        pivot = row_all(cols[0], 0)
        for j in range(8):
            root = lax.rsqrt(pivot)
            if j < 7:
                pivot = row_all(cols[j + 1], j + 1) - (row_all(cols[j], j + 1) * root) * (row_all(cols[j + 1], j) * root)
            scaled = cols[j] * root
            below = jnp.where(sub > j, scaled, 0.0)
            here = lane == 8 * g + j
            row = row_all(jnp.where(here, 1.0, r), j) * root
            r = jnp.where(sub == j, row, jnp.where(here & (sub > j), 0.0, r) - below * row)
            ups = {}
            for l in range(j + 1, 8):
                ups[l] = row_all(cols[l], j) * root
                cols[l] = cols[l] - scaled * ups[l]
            inverse_row = jnp.where((lane > 8 * g + j) & (lane < 8 * g + 8), 0.0, row)
            for i in near:
                c = raw[i]
                m = c[j] * root
                for l in range(j + 1, 8):
                    c[l] = c[l] - m * ups[l]
                accs[i] = accs[i] - m * inverse_row
                if i == g + 1:
                    ahead = [ahead[l] - m * row_all(m, l) for l in range(8)]
        w[g] = r
        for i in near:
            w[i] = accs[i]
        if g + 1 == end and end < count:
            xs, ys = [], []
            for i in range(start, end):
                xs.append(jnp.where(lane >= 8 * end, w[i], 0.0))
                ys.append(jnp.where((lane < 8 * end) & (lane > 8 * i + sub), 0.0, w[i]))
            xh, xl = split(jnp.concatenate(xs, axis=0))
            yh, yl = split(jnp.concatenate(ys, axis=0))
            delta = lax.dot_general(
                jnp.concatenate([xh, xl, xh], axis=0),
                jnp.concatenate([yh, yh, yl], axis=0),
                (((0,), (0,)), ((), ())),
                preferred_element_type=F32,
            )
            done = (lane >= 8 * start) & (lane < 8 * end)
            for i in range(end, count):
                w[i] = jnp.where(done, 0.0, w[i]) - delta[8 * i : 8 * i + 8]
            start = end
        cols = ahead
        fill(g)
    return w


def aligned(x, m=16):
    return pl.multiple_of(x, m)


def stacked(hi, lo):
    return jnp.concatenate(
        [jnp.concatenate([hi, hi], axis=1), jnp.concatenate([lo, jnp.zeros_like(lo)], axis=1)], axis=0
    )


def fold(o):
    return o[:, :BS] + o[:, BS:]


def chol_kernel(plan_ref, mat_ref, out_ref, sol_ref, a_ref, hi_ref, lo_ref, inv_ref, winv_ref, wnext_ref, y_ref):
    n = G // BS
    for t, (i, j) in enumerate(TILES):
        a_ref[i * SB : (i + 1) * SB, j * SB : (j + 1) * SB] = mat_ref[t * SB : (t + 1) * SB, :]
    a_ref[pl.ds(G, EXTRA), :] = jnp.zeros((EXTRA, G), F32)
    for j in range(NS):
        t = TILES.index((j, j)) * SB
        for h in range(2):
            a_ref[G : G + 1, j * SB + h * BS : j * SB + (h + 1) * BS] = mat_ref[t + h : t + h + 1, BS:]
    lane2 = lax.broadcasted_iota(jnp.int32, (BS, BS), 1)
    sub2 = lax.broadcasted_iota(jnp.int32, (BS, BS), 0)
    ext = pl.ds(G, EXTRA)

    def put(rows, cols, o):
        oh, ol = split(o)
        hi_ref[rows, cols] = oh
        lo_ref[rows, cols] = ol
        return jnp.concatenate([oh, ol], axis=1)

    def solved(rows_list, cols):
        x = jnp.concatenate([a_ref[rows, cols] for rows in rows_list], axis=0)
        xh, xl = split(x)
        return fold(dot_nt(jnp.concatenate([xh, xl], axis=1), winv_ref[...]))

    def update(rows, erows, jc, pc):
        xh = jnp.concatenate([hi_ref[rows, pc], hi_ref[ext, pc]], axis=0)
        xl = jnp.concatenate([lo_ref[rows, pc], lo_ref[ext, pc]], axis=0)
        rh, rl = hi_ref[jc, pc], lo_ref[jc, pc]
        o = dot_nt(xh, rh) + dot_nt(xl, rh) + dot_nt(xh, rl)
        a_ref[rows, jc] = a_ref[rows, jc] - o[:SB]
        a_ref[erows, jc] = a_ref[erows, jc] - o[SB:]

    def step(sides, count, k, carry):
        at = aligned(k * BS, BS)
        cols = pl.ds(at, BS)
        odd = lax.rem(k, 2)
        prev = pl.ds(aligned(jnp.maximum(k - 1, 0) * BS, BS), BS)
        edummy = DUMMY + SB
        eside = pl.ds(aligned(jnp.where(odd == 1, G, edummy)), EXTRA)

        waiting = {}

        def solve_side(t):
            rows = pl.ds(aligned(plan_ref[k, t]), SB)
            o = solved([rows, eside] if t == 0 else [rows], prev)
            both = put(rows, prev, o[:SB])
            if t == 0:
                both = jnp.concatenate([both, put(eside, prev, o[SB:])], axis=0)
            waiting[t] = both

        def update_side(t):
            d = fold(dot_nt(waiting.pop(t), wnext_ref[...]))
            rows = pl.ds(aligned(jnp.where(odd == 1, plan_ref[k, t], DUMMY)), SB)
            a_ref[rows, cols] = a_ref[rows, cols] - d[:SB]
            if t == 0:
                a_ref[eside, cols] = a_ref[eside, cols] - d[SB:]

        def tile_update(t):
            u = SIDES + 4 * t
            rows = pl.ds(aligned(plan_ref[k, u]), SB)
            jc = pl.ds(aligned(plan_ref[k, u + 1], SB), SB)
            pc = pl.ds(aligned(plan_ref[k, u + 2], SB), SB)
            update(rows, pl.ds(aligned(jnp.where(plan_ref[k, u + 3] == 1, G, edummy)), EXTRA), jc, pc)

        def fill(g):
            for t in range(sides):
                if t // SOLVES == g:
                    solve_side(t)
            for t in range(sides):
                if t // SOLVES + LAG == g:
                    update_side(t)
            if FIRST_UNIT <= g < FIRST_UNIT + count:
                tile_update(g - FIRST_UNIT)

        block = a_ref[pl.ds(at, BS), cols]
        w = eliminate([block[8 * i : 8 * i + 8] for i in range(BS // 8)], fill)
        w = jnp.concatenate(w, axis=0)
        inv = jnp.where(lane2 <= sub2, w, 0.0)
        inv_ref[pl.ds(at, BS), :] = inv
        ih, il = split(inv)
        winv_ref[...] = stacked(ih, il)

        @pl.when(odd == 0)
        def _():
            nxt = pl.ds(aligned(at + BS, BS), BS)
            o = solved([nxt], cols)
            both = put(nxt, cols, o)
            weights = stacked(both[:, :BS], both[:, BS:])
            wnext_ref[...] = weights
            a_ref[nxt, nxt] = a_ref[nxt, nxt] - fold(dot_nt(both, weights))

        @pl.when((odd == 1) & (k < n - 1))
        def _():
            nxt = pl.ds(aligned(at + BS, BS), SB)
            o = solved([nxt, ext], cols)
            put(nxt, cols, o[:SB])
            put(ext, cols, o[SB:])
            update(nxt, ext, nxt, pl.ds(aligned(at - BS, SB), SB))

        @pl.when(k == n - 1)
        def _():
            put(ext, cols, solved([ext], cols))

        a_ref[pl.ds(at, BS), cols] = jnp.where(lane2 == sub2, 1.0 / w, jnp.where(lane2 > sub2, w, 0.0)).T
        return carry

    for first, last, sides, count in SEGMENTS:
        lax.fori_loop(first, last, functools.partial(step, sides, count), 0)

    def column(row):
        return jnp.broadcast_to(row, (BS, BS)).T

    def back(s, c):
        k = n - 1 - s
        at = aligned(k * BS, BS)
        cols = pl.ds(at, BS)
        z = jnp.sum(column(y_ref[0:1, cols]) * inv_ref[pl.ds(at, BS), :], axis=0, keepdims=True)
        sol_ref[pl.ds(k, 1), :] = z
        zc = column(z)

        def sub(j, c2):
            jc = pl.ds(aligned(j * SB, SB), SB)
            block = hi_ref[pl.ds(at, BS), jc].astype(F32) + lo_ref[pl.ds(at, BS), jc].astype(F32)
            y_ref[0:1, jc] = y_ref[0:1, jc] - jnp.sum(jnp.concatenate([zc, zc], axis=1) * block, axis=0, keepdims=True)
            return c2

        lax.fori_loop(0, (k + 1) // 2, sub, 0)
        return c

    y_ref[...] = hi_ref[ext, :].astype(F32)[:8] + lo_ref[ext, :].astype(F32)[:8]
    lax.fori_loop(0, n, back, 0)

    p, q = lax.axis_index("gx"), lax.axis_index("gy")
    for r in range(2):
        for c in range(2):
            rb = r * 8 + p
            cb = c * 8 + q
            rows = pl.ds(aligned(rb * BS, BS), BS)
            cols = pl.ds(aligned(cb * BS, BS), BS)
            off = hi_ref[rows, cols].astype(F32) + lo_ref[rows, cols].astype(F32)
            out_ref[r, :, c, :] = jnp.where(rb > cb, off, jnp.where(rb == cb, a_ref[rows, cols], 0.0))


def cholesky_call(payload):
    return pl.pallas_call(
        chol_kernel,
        out_shape=(jax.ShapeDtypeStruct((2, BS, 2, BS), F32), jax.ShapeDtypeStruct((G // BS, BS), F32)),
        in_specs=[
            pl.BlockSpec(memory_space=pltpu.SMEM),
            pl.BlockSpec(memory_space=pltpu.VMEM),
        ],
        out_specs=(pl.BlockSpec(memory_space=pltpu.VMEM), pl.BlockSpec(memory_space=pltpu.VMEM)),
        scratch_shapes=[
            pltpu.VMEM((TALL, G), F32),
            pltpu.VMEM((TALL, G), BF16),
            pltpu.VMEM((TALL, G), BF16),
            pltpu.VMEM((G, BS), F32),
            pltpu.VMEM((SB, SB), BF16),
            pltpu.VMEM((SB, SB), BF16),
            pltpu.VMEM((8, G), F32),
        ],
        compiler_params=pltpu.CompilerParams(vmem_limit_bytes=CHOL_MB * 1024 * 1024),
        name="chol",
    )(jnp.asarray(plan(), jnp.int32), payload)


def on_device(total, blocks, coefficients, residuals):
    payload = reduce_call(blocks, coefficients, residuals, 1.0 / total)
    factor, answer = cholesky_call(payload)
    return factor.reshape(1, 2, BS, 1, 2, BS), answer


def solution(mesh):
    def whole(blocks, coefficients, residuals):
        spread = P(("gx", "gy", "gz"))
        return jax.shard_map(
            functools.partial(on_device, blocks.shape[0]),
            mesh=mesh,
            in_specs=(spread, spread, spread),
            out_specs=(P("gx", None, None, "gy", None, None), P()),
            check_vma=False,
        )(blocks, coefficients, residuals)

    return whole
```

```python
import functools

import jax
import jax.numpy as jnp
from jax import lax
from jax.experimental import pallas as pl
from jax.experimental.pallas import tpu as pltpu
from jax.sharding import PartitionSpec as P

G = 2048
BS = 128
SB = 2 * BS
NS = G // SB
EXTRA = 16
F32 = jnp.float32
BF16 = jnp.bfloat16
MESH = pl.DeviceIdType.MESH
ROUNDS = 3
SKEW = 1
RED_MB = 35
CHOL_MB = 44
STAGES = 9
STREAMS = 3 * ROUNDS
DIAG = [(j, j) for j in range(NS)]
SIDE = [(i, j) for j in range(NS) for i in range(j + 1, NS)]
TILES = DIAG[0::2] + SIDE[0::2] + DIAG[1::2] + SIDE[1::2]
ROWS = len(TILES) * SB
HALF = ROWS // 2
PART = HALF // STREAMS
UNITS_OF = (PART // 4, PART // 16)
ORDERS = ("xyz", "yzx", "zxy")


def split(x):
    hi = x.astype(BF16)
    return hi, (x - hi.astype(F32)).astype(BF16)


def dot_nt(a, b):
    return lax.dot_general(a, b, (((1,), (1,)), ((), ())), preferred_element_type=F32)


def dot_nn(a, b):
    return lax.dot_general(a, b, (((1,), (0,)), ((), ())), preferred_element_type=F32)


def lane_all(x, lane):
    return jnp.broadcast_to(x[:, lane : lane + 1], x.shape)


def row_all(x, row):
    return jnp.broadcast_to(x[row : row + 1, :], x.shape)


def place_of(x, y, z, core):
    return (lax.rem(y, 2) * 4 + x, z * 2 + core, y // 2)


def reduce_kernel(scale, blk_ref, coef_ref, res_ref, pay, design, flipped, outbox, inbox, work, near, far, ring, swap_sem, rs_sem, ag_sem, end_sem):
    gx, gy, gz = lax.axis_index("gx"), lax.axis_index("gy"), lax.axis_index("gz")
    at = {"x": lax.rem(gx, 4), "y": gz * 2 + gx // 4, "z": gy // 2}
    core = lax.rem(gy, 2)

    def device(axis, shift):
        c = dict(at)
        c[axis] = lax.rem(c[axis] + shift + 4, 4)
        return place_of(c["x"], c["y"], c["z"], core)

    twin = place_of(at["x"], at["y"], at["z"], 1 - core)
    barrier = pltpu.get_barrier_semaphore()
    for axis in "xyz":
        for shift in (1, 2, 3):
            pl.semaphore_signal(barrier, inc=1, device_id=device(axis, shift), device_id_type=MESH)
    pl.semaphore_signal(barrier, inc=1, device_id=twin, device_id_type=MESH)

    slots, obs = blk_ref.shape
    step = 256

    def place(t, c):
        rows = pl.ds(pl.multiple_of(t * step, step), step)
        ids = [jnp.broadcast_to(blk_ref[s : s + 1, rows], (BS, step)).T for s in range(slots)]
        vals = [coef_ref[rows, s * BS : (s + 1) * BS].astype(F32) for s in range(slots)]
        for b in range(G // BS):
            d = jnp.zeros((step, BS), F32)
            for s in range(slots):
                d = jnp.where(ids[s] == b, vals[s], d)
            db = d.astype(BF16)
            design[rows, b * BS : (b + 1) * BS] = db
            flipped[b * BS : (b + 1) * BS, rows] = db.T
        return c

    lax.fori_loop(0, obs // step, place, 0)

    res = res_ref[...]
    r1 = res.astype(BF16).astype(F32)
    r2 = (res - r1).astype(BF16).astype(F32)
    r3 = res - r1 - r2
    first = lax.broadcasted_iota(jnp.int32, (8, obs), 0)
    lhs = jnp.where(first == 0, r1, jnp.where(first == 1, r2, jnp.where(first == 2, r3, 0.0))).astype(BF16)

    def ds(start, size):
        return pl.ds(pl.multiple_of(start, 8), size)

    mine = core * HALF

    def gram(side, slot, dst, plus=None):
        (i0, j0), (i1, j1) = TILES[slot], TILES[slot + len(TILES) // 2]
        i = (i0 + (i1 - i0) * side) * SB
        j = (j0 + (j1 - j0) * side) * SB
        cols = design[:, pl.ds(pl.multiple_of(j, SB), SB)]
        base = slot * SB
        tile = dot_nn(flipped[pl.ds(pl.multiple_of(i, SB), SB), :], cols) * scale
        dst[base : base + SB, :] = tile if plus is None else tile + plus[base : base + SB, :]
        if i0 == j0:
            row = jnp.sum(dot_nn(lhs, cols), axis=0, keepdims=True) * scale
            rows = jnp.concatenate([row[:, :BS], row[:, BS:], jnp.zeros((6, BS), F32)], axis=0)
            dst[base : base + 8, BS:] = rows if plus is None else rows + plus[base : base + 8, BS:]

    started = []

    def remote(src, dst, sems, to):
        copy = pltpu.make_async_remote_copy(
            src_ref=src, dst_ref=dst, send_sem=sems.at[0], recv_sem=sems.at[1], device_id=to, device_id_type=MESH
        )
        copy.start()
        started.append(copy)
        return copy

    def add(dst, dst_start, srcs, src_start, size, goal=None):
        piece = min(size, 64)
        goal, goal_start = (dst, dst_start) if goal is None else goal

        def body(t, carry):
            total = dst[ds(dst_start + t * piece, piece), :]
            for src in srcs:
                total = total + src[ds(src_start + t * piece, piece), :]
            goal[ds(goal_start + t * piece, piece), :] = total
            return carry

        if size == piece:
            body(0, 0)
        else:
            lax.fori_loop(0, size // piece, body, 0)

    class Stream:
        def __init__(self, s):
            self.s = s
            self.order = ORDERS[s % 3]
            self.base = s * PART
            self.pieces = []

        def swap(self):
            rows = PART * self.s
            self.swapped = remote(outbox.at[ds(rows, PART)], inbox.at[ds(rows, PART)], swap_sem.at[self.s], twin)

        def opposite(self):
            s, unit = self.s, UNITS_OF[0]
            piece, axis = self.enter(0), self.order[0]
            half = unit // 2
            self.a = remote(work.at[ds(piece(2), half)], near.at[s, ds(0, half)], rs_sem.at[s, 0, 0], device(axis, 1))
            self.b = remote(
                work.at[ds(piece(2) + half, half)], near.at[s, ds(half, half)], rs_sem.at[s, 0, 1], device(axis, -1)
            )

        def enter(self, p):
            m, base, unit = at[self.order[p]], self.base, UNITS_OF[p]
            self.pieces.append(lambda i: base + lax.rem(m + i + 4, 4) * unit)
            return self.pieces[p]

        def sides(self):
            s, unit, axis, piece = self.s, UNITS_OF[0], self.order[0], self.pieces[0]
            half = unit // 2
            self.a.wait_recv()
            add(work, piece(1), (near.at[s],), 0, half)
            u = remote(work.at[ds(piece(1), unit)], far.at[s, 0, ds(0, unit)], rs_sem.at[s, 0, 2], device(axis, 1))
            self.b.wait_recv()
            add(work, piece(-1) + half, (near.at[s],), half, half)
            d = remote(work.at[ds(piece(-1), unit)], far.at[s, 1, ds(0, unit)], rs_sem.at[s, 0, 3], device(axis, -1))
            self.wait = (u, d)

        def finish(self, p):
            for copy in self.wait:
                copy.wait_recv()
            self.base = self.pieces[p](0)
            srcs = tuple(far.at[self.s, k] for k in range(len(self.wait)))
            add(work, self.base, srcs, sum(UNITS_OF[:p]), UNITS_OF[p])

        def exchange(self):
            self.finish(0)
            s, unit, piece, axis = self.s, UNITS_OF[1], self.enter(1), self.order[1]
            off = UNITS_OF[0]
            self.wait = tuple(
                remote(work.at[ds(piece(i), unit)], far.at[s, i - 1, ds(off, unit)], rs_sem.at[s, 1, i - 1], device(axis, i))
                for i in (1, 2, 3)
            )

        def share(self):
            self.finish(1)
            s, unit, axis = self.s, UNITS_OF[1], self.order[2]
            own = work.at[ds(self.base, unit)]
            ring[s, at[axis]] = own[...]
            self.wait = tuple(
                remote(own, ring.at[s, at[axis]], rs_sem.at[s, 2, i - 1], device(axis, i)) for i in (1, 2, 3)
            )

        def spread(self, p):
            s, unit, axis, piece = self.s, UNITS_OF[p], self.order[p], self.pieces[p]
            for copy in self.wait:
                copy.wait_recv()
            if p == 1:
                pay[ds(mine + self.base, unit), :] = ((ring[s, 0] + ring[s, 1]) + ring[s, 2]) + ring[s, 3]
            own = pay.at[ds(mine + piece(0), unit)]
            shifts = (1, 2, 3) if p else (1, 3)
            self.wait = tuple(remote(own, own, ag_sem.at[s, p, i - 1], device(axis, i)) for i in shifts)
            if p == 0:
                self.ends = [remote(own, own, end_sem.at[s, 0], twin)]

        def relay(self):
            s, unit, axis, piece = self.s, UNITS_OF[0], self.order[0], self.pieces[0]
            half = unit // 2
            u, d = self.wait
            u.wait_recv()
            part = pay.at[ds(mine + piece(-1), half)]
            up = remote(part, part, ag_sem.at[s, 0, 1], device(axis, 1))
            d.wait_recv()
            part = pay.at[ds(mine + piece(1) + half, half)]
            down = remote(part, part, ag_sem.at[s, 0, 3], device(axis, -1))
            self.wait = (up, down)
            for k, i in ((1, -1), (2, 1)):
                part = pay.at[ds(mine + piece(i), unit)]
                self.ends.append(remote(part, part, end_sem.at[s, k], twin))

        def tail(self):
            for copy in self.wait:
                copy.wait_recv()
            part = pay.at[ds(mine + self.pieces[0](2), UNITS_OF[0])]
            self.ends.append(remote(part, part, end_sem.at[self.s, 3], twin))

        def end(self):
            for copy in self.ends:
                copy.wait_recv()

        def run(self, stage):
            if stage == 0:
                self.opposite()
            elif stage == 1:
                self.sides()
            elif stage == 2:
                self.exchange()
            elif stage == 3:
                self.share()
            elif stage < 6:
                self.spread(5 - stage)
            elif stage == 6:
                self.relay()
            elif stage == 7:
                self.tail()
            else:
                self.end()

    streams = [Stream(s) for s in range(STREAMS)]
    per = PART // SB

    def give(r):
        for s in range(3 * r, 3 * r + 3):
            for k in range(per):
                gram(1 - core, s * per + k, outbox)
            if s == 0:
                pl.semaphore_wait(barrier, 10)
            streams[s].swap()

    def keep(r):
        for s in range(3 * r, 3 * r + 3):
            streams[s].swapped.wait_recv()
            for k in range(per):
                gram(core, s * per + k, work, inbox)
            streams[s].run(0)

    give(0)
    for t in range(STAGES + SKEW * (ROUNDS - 1)):
        for r in reversed(range(ROUNDS)):
            stage = t - SKEW * r
            if stage == 0:
                if r + 1 < ROUNDS:
                    give(r + 1)
                keep(r)
            elif 0 < stage < STAGES:
                for c in range(3):
                    streams[3 * r + c].run(stage)
    for copy in started:
        copy.wait_send()


def reduce_call(blocks, coefficients, residuals, scale):
    obs = blocks.shape[0]
    units = sum(UNITS_OF)
    return pl.pallas_call(
        functools.partial(reduce_kernel, scale),
        out_shape=jax.ShapeDtypeStruct((ROWS, SB), F32),
        in_specs=[pl.BlockSpec(memory_space=pltpu.VMEM)] * 3,
        out_specs=pl.BlockSpec(memory_space=pltpu.VMEM),
        scratch_shapes=[
            pltpu.VMEM((obs, G), BF16),
            pltpu.VMEM((G, obs), BF16),
            pltpu.VMEM((HALF, SB), F32),
            pltpu.VMEM((HALF, SB), F32),
            pltpu.VMEM((HALF, SB), F32),
            pltpu.VMEM((STREAMS, UNITS_OF[0], SB), F32),
            pltpu.VMEM((STREAMS, 3, units, SB), F32),
            pltpu.VMEM((STREAMS, 4, UNITS_OF[1], SB), F32),
            pltpu.SemaphoreType.DMA((STREAMS, 2)),
            pltpu.SemaphoreType.DMA((STREAMS, 3, 4, 2)),
            pltpu.SemaphoreType.DMA((STREAMS, 3, 4, 2)),
            pltpu.SemaphoreType.DMA((STREAMS, 4, 2)),
        ],
        compiler_params=pltpu.CompilerParams(
            vmem_limit_bytes=RED_MB * 1024 * 1024, collective_id=0, has_side_effects=True
        ),
        name="reduce",
    )(blocks.T, coefficients.reshape(obs, -1), residuals.reshape(1, obs))


SPLITS = (5, 10, 16)
DUMMY = G + EXTRA
TALL = DUMMY + SB + EXTRA
SEGMENTS = ((0, 8, 7, 7), (8, 14, 3, 6), (14, 16, 1, 0))
UNITS = 7
SOLVES = 2
LAG = 2
UNIT_AT = (9, 9, 9, 10, 10, 10, 11)
SIDES = NS - 1


def plan():
    n = 2 * NS
    sides = [[DUMMY] * SIDES for _ in range(n)]
    units = [[(DUMMY, 0, 0, 0)] * UNITS for _ in range(n)]
    todo = []
    for k in range(n):
        if k:
            first = (k - 1) // 2 + (1 if k % 2 else 2)
            for t, i in enumerate(range(first, NS)):
                sides[k][t] = i * SB
        if k >= 2 and k % 2 == 0:
            p = k // 2 - 1
            for j in range(p + 1, NS):
                for i in range(j, NS):
                    if (i, j) != (p + 1, p + 1):
                        todo.append((2 * j if i > j else 2 * j - 1, j, p, i))
        todo.sort()
        room = next(u for a, b, _, u in SEGMENTS if a <= k < b)
        now, todo = todo[:room], todo[room:]
        for t, (limit, j, p, i) in enumerate(now):
            assert limit >= k
            units[k][t] = (i * SB, j * SB, p * SB, 1 if i == j else 0)
    assert not todo
    flat = []
    for k in range(n):
        flat.append(sides[k] + [v for u in units[k] for v in u])
    return flat


def eliminate(w, fill):
    lane = lax.broadcasted_iota(jnp.int32, (8, BS), 1)
    sub = lax.broadcasted_iota(jnp.int32, (8, BS), 0)
    w = list(w)
    count = len(w)
    start = 0
    for g in range(count):
        end = min(e for e in SPLITS if e > g)
        if g == start:
            cols = [lane_all(w[g], 8 * g + j) for j in range(8)]
        r = w[g]
        group = (lane >= 8 * g) & (lane < 8 * g + 8)
        near = range(g + 1, end)
        raw = {i: [lane_all(w[i], 8 * g + j) for j in range(8)] for i in near}
        ahead = [lane_all(w[g + 1], 8 * g + 8 + j) for j in range(8)] if g + 1 < end else None
        accs = {i: jnp.where(group, 0.0, w[i]) for i in near}
        pivot = row_all(cols[0], 0)
        for j in range(8):
            root = lax.rsqrt(pivot)
            if j < 7:
                pivot = row_all(cols[j + 1], j + 1) - (row_all(cols[j], j + 1) * root) * (row_all(cols[j + 1], j) * root)
            scaled = cols[j] * root
            below = jnp.where(sub > j, scaled, 0.0)
            here = lane == 8 * g + j
            row = row_all(jnp.where(here, 1.0, r), j) * root
            r = jnp.where(sub == j, row, jnp.where(here & (sub > j), 0.0, r) - below * row)
            ups = {}
            for l in range(j + 1, 8):
                ups[l] = row_all(cols[l], j) * root
                cols[l] = cols[l] - scaled * ups[l]
            inverse_row = jnp.where((lane > 8 * g + j) & (lane < 8 * g + 8), 0.0, row)
            for i in near:
                c = raw[i]
                m = c[j] * root
                for l in range(j + 1, 8):
                    c[l] = c[l] - m * ups[l]
                accs[i] = accs[i] - m * inverse_row
                if i == g + 1:
                    ahead = [ahead[l] - m * row_all(m, l) for l in range(8)]
        w[g] = r
        for i in near:
            w[i] = accs[i]
        if g + 1 == end and end < count:
            xs, ys = [], []
            for i in range(start, end):
                xs.append(jnp.where(lane >= 8 * end, w[i], 0.0))
                ys.append(jnp.where((lane < 8 * end) & (lane > 8 * i + sub), 0.0, w[i]))
            xh, xl = split(jnp.concatenate(xs, axis=0))
            yh, yl = split(jnp.concatenate(ys, axis=0))
            delta = lax.dot_general(
                jnp.concatenate([xh, xl, xh], axis=0),
                jnp.concatenate([yh, yh, yl], axis=0),
                (((0,), (0,)), ((), ())),
                preferred_element_type=F32,
            )
            done = (lane >= 8 * start) & (lane < 8 * end)
            for i in range(end, count):
                w[i] = jnp.where(done, 0.0, w[i]) - delta[8 * i : 8 * i + 8]
            start = end
        cols = ahead
        fill(g)
    return w


def aligned(x, m=16):
    return pl.multiple_of(x, m)


def stacked(hi, lo):
    return jnp.concatenate(
        [jnp.concatenate([hi, hi], axis=1), jnp.concatenate([lo, jnp.zeros_like(lo)], axis=1)], axis=0
    )


def fold(o):
    return o[:, :BS] + o[:, BS:]


def chol_kernel(plan_ref, mat_ref, out_ref, sol_ref, a_ref, hi_ref, lo_ref, inv_ref, winv_ref, wnext_ref, y_ref):
    n = G // BS
    for t, (i, j) in enumerate(TILES):
        a_ref[i * SB : (i + 1) * SB, j * SB : (j + 1) * SB] = mat_ref[t * SB : (t + 1) * SB, :]
    a_ref[pl.ds(G, EXTRA), :] = jnp.zeros((EXTRA, G), F32)
    for j in range(NS):
        t = TILES.index((j, j)) * SB
        for h in range(2):
            a_ref[G : G + 1, j * SB + h * BS : j * SB + (h + 1) * BS] = mat_ref[t + h : t + h + 1, BS:]
    lane2 = lax.broadcasted_iota(jnp.int32, (BS, BS), 1)
    sub2 = lax.broadcasted_iota(jnp.int32, (BS, BS), 0)
    ext = pl.ds(G, EXTRA)

    def put(rows, cols, o):
        oh, ol = split(o)
        hi_ref[rows, cols] = oh
        lo_ref[rows, cols] = ol
        return jnp.concatenate([oh, ol], axis=1)

    def solved(rows_list, cols):
        x = jnp.concatenate([a_ref[rows, cols] for rows in rows_list], axis=0)
        xh, xl = split(x)
        return fold(dot_nt(jnp.concatenate([xh, xl], axis=1), winv_ref[...]))

    def update(rows, erows, jc, pc):
        xh = jnp.concatenate([hi_ref[rows, pc], hi_ref[ext, pc]], axis=0)
        xl = jnp.concatenate([lo_ref[rows, pc], lo_ref[ext, pc]], axis=0)
        rh, rl = hi_ref[jc, pc], lo_ref[jc, pc]
        o = dot_nt(xh, rh) + dot_nt(xl, rh) + dot_nt(xh, rl)
        a_ref[rows, jc] = a_ref[rows, jc] - o[:SB]
        a_ref[erows, jc] = a_ref[erows, jc] - o[SB:]

    def step(sides, count, k, carry):
        at = aligned(k * BS, BS)
        cols = pl.ds(at, BS)
        odd = lax.rem(k, 2)
        prev = pl.ds(aligned(jnp.maximum(k - 1, 0) * BS, BS), BS)
        edummy = DUMMY + SB
        eside = pl.ds(aligned(jnp.where(odd == 1, G, edummy)), EXTRA)

        waiting = {}

        def solve_side(t):
            rows = pl.ds(aligned(plan_ref[k, t]), SB)
            o = solved([rows, eside] if t == 0 else [rows], prev)
            both = put(rows, prev, o[:SB])
            if t == 0:
                both = jnp.concatenate([both, put(eside, prev, o[SB:])], axis=0)
            waiting[t] = both

        def update_side(t):
            d = fold(dot_nt(waiting.pop(t), wnext_ref[...]))
            rows = pl.ds(aligned(jnp.where(odd == 1, plan_ref[k, t], DUMMY)), SB)
            a_ref[rows, cols] = a_ref[rows, cols] - d[:SB]
            if t == 0:
                a_ref[eside, cols] = a_ref[eside, cols] - d[SB:]

        def tile_update(t):
            u = SIDES + 4 * t
            rows = pl.ds(aligned(plan_ref[k, u]), SB)
            jc = pl.ds(aligned(plan_ref[k, u + 1], SB), SB)
            pc = pl.ds(aligned(plan_ref[k, u + 2], SB), SB)
            update(rows, pl.ds(aligned(jnp.where(plan_ref[k, u + 3] == 1, G, edummy)), EXTRA), jc, pc)

        def fill(g):
            for t in range(sides):
                if t // SOLVES == g:
                    solve_side(t)
            for t in range(sides):
                if t // SOLVES + LAG == g:
                    update_side(t)
            for t in range(count):
                if UNIT_AT[t] == g:
                    tile_update(t)

        block = a_ref[pl.ds(at, BS), cols]
        w = eliminate([block[8 * i : 8 * i + 8] for i in range(BS // 8)], fill)
        w = jnp.concatenate(w, axis=0)
        inv = jnp.where(lane2 <= sub2, w, 0.0)
        inv_ref[pl.ds(at, BS), :] = w
        ih, il = split(inv)
        winv_ref[...] = stacked(ih, il)

        @pl.when(odd == 0)
        def _():
            nxt = pl.ds(aligned(at + BS, BS), BS)
            o = solved([nxt], cols)
            both = put(nxt, cols, o)
            weights = stacked(both[:, :BS], both[:, BS:])
            wnext_ref[...] = weights
            a_ref[nxt, nxt] = a_ref[nxt, nxt] - fold(dot_nt(both, weights))

        @pl.when((odd == 1) & (k < n - 1))
        def _():
            nxt = pl.ds(aligned(at + BS, BS), SB)
            o = solved([nxt, ext], cols)
            put(nxt, cols, o[:SB])
            put(ext, cols, o[SB:])
            update(nxt, ext, nxt, pl.ds(aligned(at - BS, SB), SB))

        @pl.when(k == n - 1)
        def _():
            put(ext, cols, solved([ext], cols))

        return carry

    for first, last, sides, count in SEGMENTS:
        lax.fori_loop(first, last, functools.partial(step, sides, count), 0)

    def column(row):
        return jnp.broadcast_to(row, (BS, BS)).T

    def back(s, c):
        k = n - 1 - s
        at = aligned(k * BS, BS)
        cols = pl.ds(at, BS)
        z = jnp.sum(column(y_ref[0:1, cols]) * jnp.where(lane2 <= sub2, inv_ref[pl.ds(at, BS), :], 0.0), axis=0, keepdims=True)
        sol_ref[pl.ds(k, 1), :] = z
        zc = column(z)

        def sub(j, c2):
            jc = pl.ds(aligned(j * SB, SB), SB)
            block = hi_ref[pl.ds(at, BS), jc].astype(F32) + lo_ref[pl.ds(at, BS), jc].astype(F32)
            y_ref[0:1, jc] = y_ref[0:1, jc] - jnp.sum(jnp.concatenate([zc, zc], axis=1) * block, axis=0, keepdims=True)
            return c2

        lax.fori_loop(0, (k + 1) // 2, sub, 0)
        return c

    y_ref[...] = hi_ref[ext, :].astype(F32)[:8] + lo_ref[ext, :].astype(F32)[:8]
    lax.fori_loop(0, n, back, 0)

    p, q = lax.axis_index("gx"), lax.axis_index("gy")
    for r in range(2):
        for c in range(2):
            rb = r * 8 + p
            cb = c * 8 + q
            rows = pl.ds(aligned(rb * BS, BS), BS)
            cols = pl.ds(aligned(cb * BS, BS), BS)
            off = hi_ref[rows, cols].astype(F32) + lo_ref[rows, cols].astype(F32)
            out_ref[r, :, c, :] = jnp.where(rb > cb, off, 0.0)

        @pl.when(p == q)
        def _(r=r):
            w = inv_ref[pl.ds(aligned((r * 8 + p) * BS, BS), BS), :]
            out_ref[r, :, r, :] = jnp.where(lane2 == sub2, 1.0 / w, jnp.where(lane2 > sub2, w, 0.0)).T


def cholesky_call(payload):
    return pl.pallas_call(
        chol_kernel,
        out_shape=(jax.ShapeDtypeStruct((2, BS, 2, BS), F32), jax.ShapeDtypeStruct((G // BS, BS), F32)),
        in_specs=[
            pl.BlockSpec(memory_space=pltpu.SMEM),
            pl.BlockSpec(memory_space=pltpu.VMEM),
        ],
        out_specs=(pl.BlockSpec(memory_space=pltpu.VMEM), pl.BlockSpec(memory_space=pltpu.VMEM)),
        scratch_shapes=[
            pltpu.VMEM((TALL, G), F32),
            pltpu.VMEM((TALL, G), BF16),
            pltpu.VMEM((TALL, G), BF16),
            pltpu.VMEM((G, BS), F32),
            pltpu.VMEM((SB, SB), BF16),
            pltpu.VMEM((SB, SB), BF16),
            pltpu.VMEM((8, G), F32),
        ],
        compiler_params=pltpu.CompilerParams(vmem_limit_bytes=CHOL_MB * 1024 * 1024),
        name="chol",
    )(jnp.asarray(plan(), jnp.int32), payload)


def on_device(total, blocks, coefficients, residuals):
    payload = reduce_call(blocks, coefficients, residuals, 1.0 / total)
    factor, answer = cholesky_call(payload)
    return factor.reshape(1, 2, BS, 1, 2, BS), answer


def solution(mesh):
    def whole(blocks, coefficients, residuals):
        spread = P(("gx", "gy", "gz"))
        return jax.shard_map(
            functools.partial(on_device, blocks.shape[0]),
            mesh=mesh,
            in_specs=(spread, spread, spread),
            out_specs=(P("gx", None, None, "gy", None, None), P()),
            check_vma=False,
        )(blocks, coefficients, residuals)

    return whole
```

```python
import functools

import jax
import jax.numpy as jnp
from jax import lax
from jax.experimental import pallas as pl
from jax.experimental.pallas import tpu as pltpu
from jax.sharding import PartitionSpec as P

G = 2048
BS = 128
SB = 2 * BS
NS = G // SB
EXTRA = 16
F32 = jnp.float32
BF16 = jnp.bfloat16
MESH = pl.DeviceIdType.MESH
ROUNDS = 3
SKEW = 1
RED_MB = 35
CHOL_MB = 44
STAGES = 9
STREAMS = 3 * ROUNDS
DIAG = [(j, j) for j in range(NS)]
SIDE = [(i, j) for j in range(NS) for i in range(j + 1, NS)]
TILES = DIAG[0::2] + SIDE[0::2] + DIAG[1::2] + SIDE[1::2]
ROWS = len(TILES) * SB
HALF = ROWS // 2
PART = HALF // STREAMS
UNITS_OF = (PART // 4, PART // 16)
ORDERS = ("xyz", "yzx", "zxy")


def split(x):
    hi = x.astype(BF16)
    return hi, (x - hi.astype(F32)).astype(BF16)


def dot_nt(a, b):
    return lax.dot_general(a, b, (((1,), (1,)), ((), ())), preferred_element_type=F32)


def dot_nn(a, b):
    return lax.dot_general(a, b, (((1,), (0,)), ((), ())), preferred_element_type=F32)


def lane_all(x, lane):
    return jnp.broadcast_to(x[:, lane : lane + 1], x.shape)


def row_all(x, row):
    return jnp.broadcast_to(x[row : row + 1, :], x.shape)


def place_of(x, y, z, core):
    return (lax.rem(y, 2) * 4 + x, z * 2 + core, y // 2)


def reduce_kernel(scale, blk_ref, coef_ref, res_ref, pay, design, flipped, outbox, inbox, work, near, far, ring, swap_sem, rs_sem, ag_sem, end_sem):
    gx, gy, gz = lax.axis_index("gx"), lax.axis_index("gy"), lax.axis_index("gz")
    at = {"x": lax.rem(gx, 4), "y": gz * 2 + gx // 4, "z": gy // 2}
    core = lax.rem(gy, 2)

    def device(axis, shift):
        c = dict(at)
        c[axis] = lax.rem(c[axis] + shift + 4, 4)
        return place_of(c["x"], c["y"], c["z"], core)

    twin = place_of(at["x"], at["y"], at["z"], 1 - core)
    barrier = pltpu.get_barrier_semaphore()
    for axis in "xyz":
        for shift in (1, 2, 3):
            pl.semaphore_signal(barrier, inc=1, device_id=device(axis, shift), device_id_type=MESH)
    pl.semaphore_signal(barrier, inc=1, device_id=twin, device_id_type=MESH)

    slots, obs = blk_ref.shape
    step = 256

    def place(t, c):
        rows = pl.ds(pl.multiple_of(t * step, step), step)
        ids = [jnp.broadcast_to(blk_ref[s : s + 1, rows], (BS, step)).T for s in range(slots)]
        vals = [coef_ref[rows, s * BS : (s + 1) * BS].astype(F32) for s in range(slots)]
        for b in range(G // BS):
            d = jnp.zeros((step, BS), F32)
            for s in range(slots):
                d = jnp.where(ids[s] == b, vals[s], d)
            db = d.astype(BF16)
            design[rows, b * BS : (b + 1) * BS] = db
            flipped[b * BS : (b + 1) * BS, rows] = db.T
        return c

    lax.fori_loop(0, obs // step, place, 0)

    res = res_ref[...]
    r1 = res.astype(BF16).astype(F32)
    r2 = (res - r1).astype(BF16).astype(F32)
    r3 = res - r1 - r2
    first = lax.broadcasted_iota(jnp.int32, (8, obs), 0)
    lhs = jnp.where(first == 0, r1, jnp.where(first == 1, r2, jnp.where(first == 2, r3, 0.0))).astype(BF16)

    def ds(start, size):
        return pl.ds(pl.multiple_of(start, 8), size)

    mine = core * HALF

    def gram(side, slot, dst, plus=None):
        (i0, j0), (i1, j1) = TILES[slot], TILES[slot + len(TILES) // 2]
        i = (i0 + (i1 - i0) * side) * SB
        j = (j0 + (j1 - j0) * side) * SB
        cols = design[:, pl.ds(pl.multiple_of(j, SB), SB)]
        base = slot * SB
        tile = dot_nn(flipped[pl.ds(pl.multiple_of(i, SB), SB), :], cols) * scale
        dst[base : base + SB, :] = tile if plus is None else tile + plus[base : base + SB, :]
        if i0 == j0:
            row = jnp.sum(dot_nn(lhs, cols), axis=0, keepdims=True) * scale
            rows = jnp.concatenate([row[:, :BS], row[:, BS:], jnp.zeros((6, BS), F32)], axis=0)
            dst[base : base + 8, BS:] = rows if plus is None else rows + plus[base : base + 8, BS:]

    started = []

    def remote(src, dst, sems, to):
        copy = pltpu.make_async_remote_copy(
            src_ref=src, dst_ref=dst, send_sem=sems.at[0], recv_sem=sems.at[1], device_id=to, device_id_type=MESH
        )
        copy.start()
        started.append(copy)
        return copy

    def add(dst, dst_start, srcs, src_start, size, goal=None):
        piece = min(size, 64)
        goal, goal_start = (dst, dst_start) if goal is None else goal

        def body(t, carry):
            total = dst[ds(dst_start + t * piece, piece), :]
            for src in srcs:
                total = total + src[ds(src_start + t * piece, piece), :]
            goal[ds(goal_start + t * piece, piece), :] = total
            return carry

        if size == piece:
            body(0, 0)
        else:
            lax.fori_loop(0, size // piece, body, 0)

    class Stream:
        def __init__(self, s):
            self.s = s
            self.order = ORDERS[s % 3]
            self.base = s * PART
            self.pieces = []

        def swap(self):
            rows = PART * self.s
            self.swapped = remote(outbox.at[ds(rows, PART)], inbox.at[ds(rows, PART)], swap_sem.at[self.s], twin)

        def opposite(self):
            s, unit = self.s, UNITS_OF[0]
            piece, axis = self.enter(0), self.order[0]
            half = unit // 2
            self.a = remote(work.at[ds(piece(2), half)], near.at[s, ds(0, half)], rs_sem.at[s, 0, 0], device(axis, 1))
            self.b = remote(
                work.at[ds(piece(2) + half, half)], near.at[s, ds(half, half)], rs_sem.at[s, 0, 1], device(axis, -1)
            )

        def enter(self, p):
            m, base, unit = at[self.order[p]], self.base, UNITS_OF[p]
            self.pieces.append(lambda i: base + lax.rem(m + i + 4, 4) * unit)
            return self.pieces[p]

        def sides(self):
            s, unit, axis, piece = self.s, UNITS_OF[0], self.order[0], self.pieces[0]
            half = unit // 2
            self.a.wait_recv()
            add(work, piece(1), (near.at[s],), 0, half)
            u = remote(work.at[ds(piece(1), unit)], far.at[s, 0, ds(0, unit)], rs_sem.at[s, 0, 2], device(axis, 1))
            self.b.wait_recv()
            add(work, piece(-1) + half, (near.at[s],), half, half)
            d = remote(work.at[ds(piece(-1), unit)], far.at[s, 1, ds(0, unit)], rs_sem.at[s, 0, 3], device(axis, -1))
            self.wait = (u, d)

        def finish(self, p):
            for copy in self.wait:
                copy.wait_recv()
            self.base = self.pieces[p](0)
            srcs = tuple(far.at[self.s, k] for k in range(len(self.wait)))
            add(work, self.base, srcs, sum(UNITS_OF[:p]), UNITS_OF[p])

        def exchange(self):
            self.finish(0)
            s, unit, piece, axis = self.s, UNITS_OF[1], self.enter(1), self.order[1]
            off = UNITS_OF[0]
            self.wait = tuple(
                remote(work.at[ds(piece(i), unit)], far.at[s, i - 1, ds(off, unit)], rs_sem.at[s, 1, i - 1], device(axis, i))
                for i in (1, 2, 3)
            )

        def share(self):
            self.finish(1)
            s, unit, axis = self.s, UNITS_OF[1], self.order[2]
            own = work.at[ds(self.base, unit)]
            ring[s, at[axis]] = own[...]
            self.wait = tuple(
                remote(own, ring.at[s, at[axis]], rs_sem.at[s, 2, i - 1], device(axis, i)) for i in (1, 2, 3)
            )

        def spread(self, p):
            s, unit, axis, piece = self.s, UNITS_OF[p], self.order[p], self.pieces[p]
            for copy in self.wait:
                copy.wait_recv()
            if p == 1:
                pay[ds(mine + self.base, unit), :] = ((ring[s, 0] + ring[s, 1]) + ring[s, 2]) + ring[s, 3]
            own = pay.at[ds(mine + piece(0), unit)]
            shifts = (1, 2, 3) if p else (1, 3)
            self.wait = tuple(remote(own, own, ag_sem.at[s, p, i - 1], device(axis, i)) for i in shifts)
            if p == 0:
                self.ends = [remote(own, own, end_sem.at[s, 0], twin)]

        def relay(self):
            s, unit, axis, piece = self.s, UNITS_OF[0], self.order[0], self.pieces[0]
            half = unit // 2
            u, d = self.wait
            u.wait_recv()
            part = pay.at[ds(mine + piece(-1), half)]
            up = remote(part, part, ag_sem.at[s, 0, 1], device(axis, 1))
            d.wait_recv()
            part = pay.at[ds(mine + piece(1) + half, half)]
            down = remote(part, part, ag_sem.at[s, 0, 3], device(axis, -1))
            self.wait = (up, down)
            for k, i in ((1, -1), (2, 1)):
                part = pay.at[ds(mine + piece(i), unit)]
                self.ends.append(remote(part, part, end_sem.at[s, k], twin))

        def tail(self):
            for copy in self.wait:
                copy.wait_recv()
            part = pay.at[ds(mine + self.pieces[0](2), UNITS_OF[0])]
            self.ends.append(remote(part, part, end_sem.at[self.s, 3], twin))

        def end(self):
            for copy in self.ends:
                copy.wait_recv()

        def run(self, stage):
            if stage == 0:
                self.opposite()
            elif stage == 1:
                self.sides()
            elif stage == 2:
                self.exchange()
            elif stage == 3:
                self.share()
            elif stage < 6:
                self.spread(5 - stage)
            elif stage == 6:
                self.relay()
            elif stage == 7:
                self.tail()
            else:
                self.end()

    streams = [Stream(s) for s in range(STREAMS)]
    per = PART // SB

    def give(r):
        for s in range(3 * r, 3 * r + 3):
            for k in range(per):
                gram(1 - core, s * per + k, outbox)
            if s == 0:
                pl.semaphore_wait(barrier, 10)
            streams[s].swap()

    def keep(r):
        for s in range(3 * r, 3 * r + 3):
            streams[s].swapped.wait_recv()
            for k in range(per):
                gram(core, s * per + k, work, inbox)
            streams[s].run(0)

    give(0)
    for t in range(STAGES + SKEW * (ROUNDS - 1)):
        for r in reversed(range(ROUNDS)):
            stage = t - SKEW * r
            if stage == 0:
                if r + 1 < ROUNDS:
                    give(r + 1)
                keep(r)
            elif 0 < stage < STAGES:
                for c in range(3):
                    streams[3 * r + c].run(stage)
    for copy in started:
        copy.wait_send()


def reduce_call(blocks, coefficients, residuals, scale):
    obs = blocks.shape[0]
    units = sum(UNITS_OF)
    return pl.pallas_call(
        functools.partial(reduce_kernel, scale),
        out_shape=jax.ShapeDtypeStruct((ROWS, SB), F32),
        in_specs=[pl.BlockSpec(memory_space=pltpu.VMEM)] * 3,
        out_specs=pl.BlockSpec(memory_space=pltpu.VMEM),
        scratch_shapes=[
            pltpu.VMEM((obs, G), BF16),
            pltpu.VMEM((G, obs), BF16),
            pltpu.VMEM((HALF, SB), F32),
            pltpu.VMEM((HALF, SB), F32),
            pltpu.VMEM((HALF, SB), F32),
            pltpu.VMEM((STREAMS, UNITS_OF[0], SB), F32),
            pltpu.VMEM((STREAMS, 3, units, SB), F32),
            pltpu.VMEM((STREAMS, 4, UNITS_OF[1], SB), F32),
            pltpu.SemaphoreType.DMA((STREAMS, 2)),
            pltpu.SemaphoreType.DMA((STREAMS, 3, 4, 2)),
            pltpu.SemaphoreType.DMA((STREAMS, 3, 4, 2)),
            pltpu.SemaphoreType.DMA((STREAMS, 4, 2)),
        ],
        compiler_params=pltpu.CompilerParams(
            vmem_limit_bytes=RED_MB * 1024 * 1024, collective_id=0, has_side_effects=True
        ),
        name="reduce",
    )(blocks.T, coefficients.reshape(obs, -1), residuals.reshape(1, obs))


SPLITS = (5, 10, 16)
DUMMY = G + EXTRA
TALL = DUMMY + SB + EXTRA
SEGMENTS = ((0, 2, 7, 0), (2, 8, 6, 7), (8, 14, 3, 6), (14, 16, 1, 0))
UNITS = 7
SOLVES = 2
LAG = 2
UNIT_AT = (9, 9, 9, 10, 10, 10, 11)
SIDES = NS - 1


def plan():
    n = 2 * NS
    sides = [[DUMMY] * SIDES for _ in range(n)]
    units = [[(DUMMY, 0, 0, 0)] * UNITS for _ in range(n)]
    todo = []
    for k in range(n):
        if k:
            first = (k - 1) // 2 + (1 if k % 2 else 2)
            for t, i in enumerate(range(first, NS)):
                sides[k][t] = i * SB
        if k >= 2 and k % 2 == 0:
            p = k // 2 - 1
            for j in range(p + 1, NS):
                for i in range(j, NS):
                    if (i, j) != (p + 1, p + 1):
                        todo.append((2 * j if i > j else 2 * j - 1, j, p, i))
        todo.sort()
        room = next(u for a, b, _, u in SEGMENTS if a <= k < b)
        now, todo = todo[:room], todo[room:]
        for t, (limit, j, p, i) in enumerate(now):
            assert limit >= k
            units[k][t] = (i * SB, j * SB, p * SB, 1 if i == j else 0)
    assert not todo
    flat = []
    for k in range(n):
        flat.append(sides[k] + [v for u in units[k] for v in u])
    return flat


def eliminate(w, fill):
    lane = lax.broadcasted_iota(jnp.int32, (8, BS), 1)
    sub = lax.broadcasted_iota(jnp.int32, (8, BS), 0)
    w = list(w)
    count = len(w)
    start = 0
    for g in range(count):
        end = min(e for e in SPLITS if e > g)
        if g == start:
            cols = [lane_all(w[g], 8 * g + j) for j in range(8)]
        r = w[g]
        group = (lane >= 8 * g) & (lane < 8 * g + 8)
        near = range(g + 1, end)
        raw = {i: [lane_all(w[i], 8 * g + j) for j in range(8)] for i in near}
        ahead = [lane_all(w[g + 1], 8 * g + 8 + j) for j in range(8)] if g + 1 < end else None
        accs = {i: jnp.where(group, 0.0, w[i]) for i in near}
        pivot = row_all(cols[0], 0)
        for j in range(8):
            root = lax.rsqrt(pivot)
            if j < 7:
                pivot = row_all(cols[j + 1], j + 1) - (row_all(cols[j], j + 1) * root) * (row_all(cols[j + 1], j) * root)
            scaled = cols[j] * root
            below = jnp.where(sub > j, scaled, 0.0)
            here = lane == 8 * g + j
            row = row_all(jnp.where(here, 1.0, r), j) * root
            r = jnp.where(sub == j, row, jnp.where(here & (sub > j), 0.0, r) - below * row)
            ups = {}
            for l in range(j + 1, 8):
                ups[l] = row_all(cols[l], j) * root
                cols[l] = cols[l] - scaled * ups[l]
            inverse_row = jnp.where((lane > 8 * g + j) & (lane < 8 * g + 8), 0.0, row)
            for i in near:
                c = raw[i]
                m = c[j] * root
                for l in range(j + 1, 8):
                    c[l] = c[l] - m * ups[l]
                accs[i] = accs[i] - m * inverse_row
                if i == g + 1:
                    ahead = [ahead[l] - m * row_all(m, l) for l in range(8)]
        w[g] = r
        for i in near:
            w[i] = accs[i]
        if g + 1 == end and end < count:
            xs, ys = [], []
            for i in range(start, end):
                xs.append(jnp.where(lane >= 8 * end, w[i], 0.0))
                ys.append(jnp.where((lane < 8 * end) & (lane > 8 * i + sub), 0.0, w[i]))
            xh, xl = split(jnp.concatenate(xs, axis=0))
            yh, yl = split(jnp.concatenate(ys, axis=0))
            delta = lax.dot_general(
                jnp.concatenate([xh, xl, xh], axis=0),
                jnp.concatenate([yh, yh, yl], axis=0),
                (((0,), (0,)), ((), ())),
                preferred_element_type=F32,
            )
            done = (lane >= 8 * start) & (lane < 8 * end)
            for i in range(end, count):
                w[i] = jnp.where(done, 0.0, w[i]) - delta[8 * i : 8 * i + 8]
            start = end
        cols = ahead
        fill(g)
    return w


def aligned(x, m=16):
    return pl.multiple_of(x, m)


def stacked(hi, lo):
    return jnp.concatenate(
        [jnp.concatenate([hi, hi], axis=1), jnp.concatenate([lo, jnp.zeros_like(lo)], axis=1)], axis=0
    )


def fold(o):
    return o[:, :BS] + o[:, BS:]


def chol_kernel(plan_ref, mat_ref, out_ref, sol_ref, a_ref, hi_ref, lo_ref, inv_ref, winv_ref, wnext_ref, y_ref):
    n = G // BS
    for t, (i, j) in enumerate(TILES):
        a_ref[i * SB : (i + 1) * SB, j * SB : (j + 1) * SB] = mat_ref[t * SB : (t + 1) * SB, :]
    a_ref[pl.ds(G, EXTRA), :] = jnp.zeros((EXTRA, G), F32)
    for j in range(NS):
        t = TILES.index((j, j)) * SB
        for h in range(2):
            a_ref[G : G + 1, j * SB + h * BS : j * SB + (h + 1) * BS] = mat_ref[t + h : t + h + 1, BS:]
    lane2 = lax.broadcasted_iota(jnp.int32, (BS, BS), 1)
    sub2 = lax.broadcasted_iota(jnp.int32, (BS, BS), 0)
    ext = pl.ds(G, EXTRA)

    def put(rows, cols, o):
        oh, ol = split(o)
        hi_ref[rows, cols] = oh
        lo_ref[rows, cols] = ol
        return jnp.concatenate([oh, ol], axis=1)

    def solved(rows_list, cols):
        x = jnp.concatenate([a_ref[rows, cols] for rows in rows_list], axis=0)
        xh, xl = split(x)
        return fold(dot_nt(jnp.concatenate([xh, xl], axis=1), winv_ref[...]))

    def update(rows, erows, jc, pc):
        xh = jnp.concatenate([hi_ref[rows, pc], hi_ref[ext, pc]], axis=0)
        xl = jnp.concatenate([lo_ref[rows, pc], lo_ref[ext, pc]], axis=0)
        rh, rl = hi_ref[jc, pc], lo_ref[jc, pc]
        o = dot_nt(xh, rh) + dot_nt(xl, rh) + dot_nt(xh, rl)
        a_ref[rows, jc] = a_ref[rows, jc] - o[:SB]
        a_ref[erows, jc] = a_ref[erows, jc] - o[SB:]

    def step(sides, count, k, carry):
        at = aligned(k * BS, BS)
        cols = pl.ds(at, BS)
        odd = lax.rem(k, 2)
        prev = pl.ds(aligned(jnp.maximum(k - 1, 0) * BS, BS), BS)
        edummy = DUMMY + SB
        eside = pl.ds(aligned(jnp.where(odd == 1, G, edummy)), EXTRA)

        waiting = {}

        def solve_side(t):
            rows = pl.ds(aligned(plan_ref[k, t]), SB)
            o = solved([rows, eside] if t == 0 else [rows], prev)
            both = put(rows, prev, o[:SB])
            if t == 0:
                both = jnp.concatenate([both, put(eside, prev, o[SB:])], axis=0)
            waiting[t] = both

        def update_side(t):
            d = fold(dot_nt(waiting.pop(t), wnext_ref[...]))
            rows = pl.ds(aligned(jnp.where(odd == 1, plan_ref[k, t], DUMMY)), SB)
            a_ref[rows, cols] = a_ref[rows, cols] - d[:SB]
            if t == 0:
                a_ref[eside, cols] = a_ref[eside, cols] - d[SB:]

        def tile_update(t):
            u = SIDES + 4 * t
            rows = pl.ds(aligned(plan_ref[k, u]), SB)
            jc = pl.ds(aligned(plan_ref[k, u + 1], SB), SB)
            pc = pl.ds(aligned(plan_ref[k, u + 2], SB), SB)
            update(rows, pl.ds(aligned(jnp.where(plan_ref[k, u + 3] == 1, G, edummy)), EXTRA), jc, pc)

        def fill(g):
            for t in range(sides):
                if t // SOLVES == g:
                    solve_side(t)
            for t in range(sides):
                if t // SOLVES + LAG == g:
                    update_side(t)
            for t in range(count):
                if UNIT_AT[t] == g:
                    tile_update(t)

        block = a_ref[pl.ds(at, BS), cols]
        w = eliminate([block[8 * i : 8 * i + 8] for i in range(BS // 8)], fill)
        w = jnp.concatenate(w, axis=0)
        inv = jnp.where(lane2 <= sub2, w, 0.0)
        inv_ref[pl.ds(at, BS), :] = w
        ih, il = split(inv)
        winv_ref[...] = stacked(ih, il)

        @pl.when(odd == 0)
        def _():
            nxt = pl.ds(aligned(at + BS, BS), BS)
            o = solved([nxt], cols)
            both = put(nxt, cols, o)
            weights = stacked(both[:, :BS], both[:, BS:])
            wnext_ref[...] = weights
            a_ref[nxt, nxt] = a_ref[nxt, nxt] - fold(dot_nt(both, weights))

        @pl.when((odd == 1) & (k < n - 1))
        def _():
            nxt = pl.ds(aligned(at + BS, BS), SB)
            o = solved([nxt, ext], cols)
            put(nxt, cols, o[:SB])
            put(ext, cols, o[SB:])
            update(nxt, ext, nxt, pl.ds(aligned(at - BS, SB), SB))

        @pl.when(k == n - 1)
        def _():
            put(ext, cols, solved([ext], cols))

        return carry

    for first, last, sides, count in SEGMENTS:
        lax.fori_loop(first, last, functools.partial(step, sides, count), 0)

    def column(row):
        return jnp.broadcast_to(row, (BS, BS)).T

    def back(s, c):
        k = n - 1 - s
        at = aligned(k * BS, BS)
        cols = pl.ds(at, BS)
        z = jnp.sum(column(y_ref[0:1, cols]) * jnp.where(lane2 <= sub2, inv_ref[pl.ds(at, BS), :], 0.0), axis=0, keepdims=True)
        sol_ref[pl.ds(k, 1), :] = z
        zc = column(z)

        def sub(j, c2):
            jc = pl.ds(aligned(j * SB, SB), SB)
            block = hi_ref[pl.ds(at, BS), jc].astype(F32) + lo_ref[pl.ds(at, BS), jc].astype(F32)
            y_ref[0:1, jc] = y_ref[0:1, jc] - jnp.sum(jnp.concatenate([zc, zc], axis=1) * block, axis=0, keepdims=True)
            return c2

        lax.fori_loop(0, (k + 1) // 2, sub, 0)
        return c

    y_ref[...] = hi_ref[ext, :].astype(F32)[:8] + lo_ref[ext, :].astype(F32)[:8]
    lax.fori_loop(0, n, back, 0)

    p, q = lax.axis_index("gx"), lax.axis_index("gy")
    for r in range(2):
        for c in range(2):
            rb = r * 8 + p
            cb = c * 8 + q
            rows = pl.ds(aligned(rb * BS, BS), BS)
            cols = pl.ds(aligned(cb * BS, BS), BS)
            off = hi_ref[rows, cols].astype(F32) + lo_ref[rows, cols].astype(F32)
            out_ref[r, :, c, :] = jnp.where(rb > cb, off, 0.0)

        @pl.when(p == q)
        def _(r=r):
            w = inv_ref[pl.ds(aligned((r * 8 + p) * BS, BS), BS), :]
            out_ref[r, :, r, :] = jnp.where(lane2 == sub2, 1.0 / w, jnp.where(lane2 > sub2, w, 0.0)).T


def cholesky_call(payload):
    return pl.pallas_call(
        chol_kernel,
        out_shape=(jax.ShapeDtypeStruct((2, BS, 2, BS), F32), jax.ShapeDtypeStruct((G // BS, BS), F32)),
        in_specs=[
            pl.BlockSpec(memory_space=pltpu.SMEM),
            pl.BlockSpec(memory_space=pltpu.VMEM),
        ],
        out_specs=(pl.BlockSpec(memory_space=pltpu.VMEM), pl.BlockSpec(memory_space=pltpu.VMEM)),
        scratch_shapes=[
            pltpu.VMEM((TALL, G), F32),
            pltpu.VMEM((TALL, G), BF16),
            pltpu.VMEM((TALL, G), BF16),
            pltpu.VMEM((G, BS), F32),
            pltpu.VMEM((SB, SB), BF16),
            pltpu.VMEM((SB, SB), BF16),
            pltpu.VMEM((8, G), F32),
        ],
        compiler_params=pltpu.CompilerParams(vmem_limit_bytes=CHOL_MB * 1024 * 1024),
        name="chol",
    )(jnp.asarray(plan(), jnp.int32), payload)


def on_device(total, blocks, coefficients, residuals):
    payload = reduce_call(blocks, coefficients, residuals, 1.0 / total)
    factor, answer = cholesky_call(payload)
    return factor.reshape(1, 2, BS, 1, 2, BS), answer


def solution(mesh):
    def whole(blocks, coefficients, residuals):
        spread = P(("gx", "gy", "gz"))
        return jax.shard_map(
            functools.partial(on_device, blocks.shape[0]),
            mesh=mesh,
            in_specs=(spread, spread, spread),
            out_specs=(P("gx", None, None, "gy", None, None), P()),
            check_vma=False,
        )(blocks, coefficients, residuals)

    return whole
```
